512 devices in a mesh: grp: 4 (over x), gx: 8 (over y, core), gy: 16 (over z).
Axes of the slice: x: 4, y: 4, z: 16, core: 2. Of those that a mesh axis runs over, the one named last changes fastest.
Arguments:
- drive: float32 [3, 64, 1024, 128], P(None, ('grp', 'gx'), 'gy'), may hold values from -6 to 6
- permeability: float32 [48, 1024, 128], P('gx', 'gy'), may hold values from 0.5 to 8
Outputs:
- state: float32 [3, 64, 1024, 128], P(None, ('grp', 'gx'), 'gy')
The draws below stay inside these ranges and needn't reach their ends.
All inputs are finite; a program needn't handle non-finite values.
Results may differ from the reference program's by a relative error of at most 0.0001.
Values sent between devices are 32-bit elements; how exact they have to be, the bound alone decides.
A program may use at most 64 MiB of HBM per device.

```python
import math
import jax
import jax.numpy as jnp
from jax import lax

CX = 2
Z = 128
SWEEPS = 4
OUTER = 2
NXD = 48
NXB = 64
NY = 1024
N_GX = 8


def steps_of(own_key, dims, split, smallest, largest):
    level, own = 1.0, jax.random.fold_in(own_key, 6)
    for axis_at, shards_of in split:
        steps = jnp.exp(jax.random.uniform(jax.random.fold_in(own, axis_at), (shards_of,), jnp.float32, smallest / len(split), largest / len(split)))
        level = level * jnp.repeat(steps, dims[axis_at] // shards_of).reshape([-1 if axis == axis_at else 1 for axis in range(len(dims))])
    return level


def scatter_about(rng, shape, deviation, limit, cuts=(), kind=jnp.bfloat16):
    result = jax.random.normal(rng, shape, jnp.float32) * deviation
    if len(cuts) > 0:
        result = steps_of(rng, shape, cuts, -0.22, 0.18) * result
    return jnp.clip(result, min=-limit, max=limit).astype(kind)


def setup_inputs(seed: int = 0) -> dict:
    streams_of = jax.random.split(jax.random.key(seed), 3)
    return {
        "drive": scatter_about(streams_of[0], (3, NXB, NY, Z), 1.0, 6.0, ((1, 32), (2, 16)), jnp.float32),
        "permeability": jnp.clip(jnp.exp(math.log(8.0) - 2.7725887 * jax.random.uniform(streams_of[1], (NXD, NY, Z), jnp.float32) ** steps_of(streams_of[1], (NXD, NY, Z), ((0, 8), (1, 16)), -0.2, 0.2)), 0.5, 8.0),
    }


relaxation = 0.8
pressure_rate = 0.5
interface_blend = 0.5


def neighbours(field, bottom):
    west_side = jnp.pad(field, ((1, 0), (0, 0), (0, 0)))[:-1]
    east_side = jnp.pad(field, ((0, 1), (0, 0), (0, 0)))[1:]
    south_side = jnp.pad(field, ((0, 0), (1, 0), (0, 0)))[:, :-1]
    north_side = jnp.pad(field, ((0, 0), (0, 1), (0, 0)))[:, 1:]
    below_side = jnp.concatenate([bottom[:, :, None], field[:, :, :-1]], axis=2)
    above_side = jnp.pad(field, ((0, 0), (0, 0), (0, 1)))[:, :, 1:]
    return west_side, east_side, south_side, north_side, below_side, above_side


def flow_sweep(fields, body_force, inflow):
    zero_plane = jnp.zeros_like(inflow)
    bottoms = (zero_plane, zero_plane, inflow, zero_plane)
    near = [neighbours(fields[component], bottoms[component]) for component in range(4)]
    pressure = fields[3]
    gradient = (near[3][1] - pressure, near[3][3] - pressure, near[3][5] - pressure)
    velocity = []
    for component in range(3):
        sides = near[component]
        laplace = sides[0] + sides[1] + sides[2] + sides[3] + sides[4] + sides[5] - 6.0 * fields[component]
        velocity.append(fields[component] + (relaxation / 6.0) * (body_force[component] + laplace - gradient[component]))
    divergence = (fields[0] - near[0][0]) + (fields[1] - near[1][2]) + (fields[2] - near[2][4])
    return [velocity[0], velocity[1], velocity[2], pressure - pressure_rate * divergence]


def bed_weights(permeability):
    extent = permeability.shape
    x_place = lax.broadcasted_iota(jnp.int32, extent, 0)
    y_place = lax.broadcasted_iota(jnp.int32, extent, 1)
    z_place = lax.broadcasted_iota(jnp.int32, extent, 2)
    sides = neighbours(permeability, jnp.zeros(extent[:2], permeability.dtype))
    west_weight = jnp.where(x_place > 0, (permeability + sides[0]) * 0.5, 0.0)
    east_weight = jnp.where(x_place < extent[0] - 1, (permeability + sides[1]) * 0.5, 0.0)
    south_weight = jnp.where(y_place > 0, (permeability + sides[2]) * 0.5, 0.0)
    north_weight = jnp.where(y_place < extent[1] - 1, (permeability + sides[3]) * 0.5, 0.0)
    below_weight = jnp.where(z_place > 0, (permeability + sides[4]) * 0.5, 0.0)
    above_weight = jnp.where(z_place < extent[2] - 1, (permeability + sides[5]) * 0.5, permeability)
    centre_weight = west_weight + east_weight + south_weight + north_weight + below_weight + above_weight
    return (west_weight, east_weight, south_weight, north_weight, below_weight, above_weight, centre_weight)


def bed_apply(field, weights):
    sides = neighbours(field, jnp.zeros(field.shape[:2], field.dtype))
    return weights[6] * field - (weights[0] * sides[0] + weights[1] * sides[1] + weights[2] * sides[2] + weights[3] * sides[3] + weights[4] * sides[4] + weights[5] * sides[5])


def bed_solve(rhs, weights):
    solution = jnp.zeros_like(rhs)
    resid = rhs
    direction = rhs
    norm_now = jnp.sum(resid * resid)
    for sweep_index in range(SWEEPS):
        bed_image = bed_apply(direction, weights)
        step_size = norm_now / jnp.sum(direction * bed_image)
        solution = solution + step_size * direction
        resid = resid - step_size * bed_image
        if sweep_index + 1 < SWEEPS:
            norm_next = jnp.sum(resid * resid)
            direction = resid + (norm_next / norm_now) * direction
            norm_now = norm_next
    return solution


def reference(drive, permeability):
    body_force = drive[:, :NXD]
    source = drive[:, NXD:].reshape(3, N_GX, CX, NY, Z).transpose(1, 0, 2, 3, 4).reshape(NXD, NY, Z)
    weights = bed_weights(permeability)
    z_place = lax.broadcasted_iota(jnp.int32, permeability.shape, 2)
    fields = [jnp.zeros((NXD, NY, Z), drive.dtype) for component in range(4)]
    inflow = jnp.zeros((NXD, NY), drive.dtype)
    surface = jnp.zeros((NXD, NY), drive.dtype)
    solution = jnp.zeros((NXD, NY, Z), drive.dtype)
    for outer_index in range(OUTER):
        rhs = source + jnp.where(z_place == Z - 1, permeability * surface[:, :, None], 0.0)
        solution = bed_solve(rhs, weights)
        for sweep_index in range(SWEEPS):
            fields = flow_sweep(fields, body_force, inflow)
        if outer_index + 1 < OUTER:
            new_inflow = permeability[:, :, -1] * (solution[:, :, -1] - surface)
            surface = interface_blend * fields[3][:, :, 0] + (1.0 - interface_blend) * surface
            inflow = new_inflow
    flow_part = jnp.stack(fields[:3])
    bed_part = solution.reshape(N_GX, 3, CX, NY, Z).transpose(1, 0, 2, 3, 4).reshape(3, N_GX * CX, NY, Z)
    return jnp.concatenate([flow_part, bed_part], axis=1)
```

```python
import functools
import jax
import jax.numpy as jnp
from jax import lax
from jax.experimental import pallas as pl
from jax.experimental.pallas import tpu as pltpu
from jax.sharding import PartitionSpec as P

MESH = pl.DeviceIdType.MESH
C = 0.8 / 6.0
CC = (0.8 / 6.0) * (0.8 / 6.0)
SCALE = 1.0 / 16.0
ROWS = 96
OWN = range(2, 10)
WIDE = range(1, 11)


def loop(lo, hi, body, carry):
    for x in range(lo, hi):
        carry = body(x, carry)
    return carry


def two_sum(a, b):
    s = a + b
    bb = s - a
    return s, (a - (s - bb)) + (b - bb)


def quick(a, b):
    s = a + b
    return s, b - (s - a)


def halves(a):
    t = a * 4097.0
    hi = t - (t - a)
    return hi, a - hi


def two_prod(a, b):
    p = a * b
    ah, al = halves(a)
    bh, bl = halves(b)
    return p, ((ah * bh - p) + ah * bl + al * bh) + al * bl


def dadd(a, b):
    s, e = two_sum(a[0], b[0])
    return quick(s, e + (a[1] + b[1]))


def dsub(a, b):
    return dadd(a, (-b[0], -b[1]))


def dmul(a, b):
    p, e = two_prod(a[0], b[0])
    return quick(p, e + (a[0] * b[1] + a[1] * b[0]))


def drecip(a):
    r = 1.0 / a[0]
    p, pe = two_prod(r, a[0])
    e = ((1.0 - p) - pe) - r * a[1]
    return quick(r, r * e)


def tree(pairs):
    pairs = list(pairs)
    while len(pairs) > 1:
        nxt = []
        for i in range(0, len(pairs) - 1, 2):
            (ah, al), (bh, bl) = pairs[i], pairs[i + 1]
            s, e = two_sum(ah, bh)
            nxt.append((s, e + (al + bl)))
        if len(pairs) % 2:
            nxt.append(pairs[-1])
        pairs = nxt
    return pairs[0]


def coefficients(mu):
    n = 4
    m = [[mu[i + j + 1] for j in range(n)] for i in range(n)]
    y = [mu[i] for i in range(n)]
    low = [[None] * n for _ in range(n)]
    inv = [None] * n
    for k in range(n):
        good = m[k][k][0] > 1e-12 * mu[2 * k + 1][0]
        safe = jnp.where(good, m[k][k][0], 1.0)
        rh, rl = drecip((safe, m[k][k][1]))
        inv[k] = (jnp.where(good, rh, 0.0), jnp.where(good, rl, 0.0))
        for i in range(k + 1, n):
            low[i][k] = dmul(m[i][k], inv[k])
        for i in range(k + 1, n):
            for j in range(k + 1, i + 1):
                m[i][j] = dsub(m[i][j], dmul(low[i][k], m[j][k]))
                m[j][i] = m[i][j]
            y[i] = dsub(y[i], dmul(low[i][k], y[k]))
    c = [None] * n
    for k in range(n - 1, -1, -1):
        s = dmul(y[k], inv[k])
        for i in range(k + 1, n):
            s = dsub(s, dmul(low[i][k], c[i]))
        c[k] = s
    return [v[0] * SCALE for v in c]


def kernel(n_grp, n_gx, n_gy, drive, perm, out, fb, e2, e3, e4, tmp, kb, w, v1, v2, v3, b2, mt, zt,
           surf, spb, infl, infs, ar1, ar2,
           lsem, hs, hr, a1s, a1r, a2s, a2r, sus, sur, ins, inr):
    grp = lax.axis_index("grp")
    gx = lax.axis_index("gx")
    gy = lax.axis_index("gy")
    flows = (n_grp - 1) * n_gx
    is_bed = grp == n_grp - 1
    j = grp * n_gx + gx
    m_of = lax.div(j, 3)
    r_of = j - 3 * m_of
    lane = lax.broadcasted_iota(jnp.int32, (8, 128), 1)
    sub = lax.broadcasted_iota(jnp.int32, (8, 128), 0)
    l0 = lane == 0
    l127 = lane == 127

    def inside(i, n):
        return (i >= 0) & (i < n)

    def held(i, n):
        return jnp.minimum(jnp.maximum(i, 0), n - 1)

    def at(flow):
        flow = held(flow, flows)
        return (lax.div(flow, n_gx), lax.rem(flow, n_gx))

    def below(f):
        return jnp.where(l0, 0.0, pltpu.roll(f, 1, 1))

    def above(f):
        return jnp.where(l127, 0.0, pltpu.roll(f, 127, 1))

    barrier = pltpu.get_barrier_semaphore()
    dirs = [(dx, dy) for dx in (-1, 0, 1) for dy in (-1, 0, 1) if (dx, dy) != (0, 0)]

    def greet(partners):
        total = jnp.int32(0)
        for ok, ident in partners:
            @pl.when(ok)
            def _(ident=ident):
                pl.semaphore_signal(barrier, inc=1, device_id=ident, device_id_type=MESH)
            total = total + ok.astype(jnp.int32)
        return total

    def run(copies):
        for ok, cp in copies:
            @pl.when(ok)
            def _(cp=cp):
                cp.start()

    def arrive(copies):
        for ok, cp in copies:
            @pl.when(ok)
            def _(cp=cp):
                cp.wait_recv()

    def drain(copies):
        for ok, cp in copies:
            @pl.when(ok)
            def _(cp=cp):
                cp.wait_send()

    def remote(src, dst, s, r, ident):
        return pltpu.make_async_remote_copy(src_ref=src, dst_ref=dst, send_sem=s, recv_sem=r,
                                            device_id=ident, device_id_type=MESH)

    def halo(e, view, first, width, wide, neighbour, exists, corners):
        sends, recvs = [], []
        for dx, dy in dirs:
            if not corners and dx != 0 and dy != 0:
                continue
            if dx == 0:
                sc, dc = (first, width), (first, width)
            elif dx == 1:
                sc, dc = (first + width - wide, wide), (first - wide, wide)
            else:
                sc, dc = (first, wide), (first + width, wide)
            if dy == 0:
                sr, dr = (16, 64), (16, 64)
            elif dy == 1:
                sr, dr = (72, 8), (8, 8)
            else:
                sr, dr = (16, 8), (80, 8)
            d = (dx + 1) * 3 + dy + 1
            cp = remote(view(sc, sr), view(dc, dr), hs.at[e, d], hr.at[e, d], neighbour(dx, dy))
            sends.append((exists(dx, dy), cp))
            recvs.append((exists(-dx, -dy), remote(view(sc, sr), view(dc, dr), hs.at[e, d], hr.at[e, d],
                                                   neighbour(-dx, -dy))))
        return sends, recvs

    @pl.when(jnp.logical_not(is_bed))
    def _():
        infl[...] = jnp.zeros_like(infl)
        load = pltpu.make_async_copy(drive, fb.at[:, 2:4, 16:80, :], lsem.at[0])
        load.start()

        def neighbour(dx, dy):
            a, b = at(j + dx)
            return (a, b, held(gy + dy, n_gy))

        def exists(dx, dy):
            return inside(j + dx, flows) & inside(gy + dy, n_gy)

        beds = []
        for dm in (-1, 0, 1):
            for dy in (-1, 0, 1):
                ok = inside(m_of + dm, n_gx) & inside(gy + dy, n_gy)
                if dm == -1:
                    ok = ok & (r_of <= 1)
                if dm == 1:
                    ok = ok & (r_of >= 1)
                beds.append((dm, dy, ok, (n_grp - 1, held(m_of + dm, n_gx), held(gy + dy, n_gy))))

        total = greet([(exists(dx, dy), neighbour(dx, dy)) for dx, dy in dirs]
                      + [(ok, ident) for _, _, ok, ident in beds])

        def clear(c0, c1, r0, r1):
            for buf in (fb, e2, e3, e4):
                buf[:, c0:c1, r0:r1, :] = jnp.zeros((buf.shape[0], c1 - c0, r1 - r0, 128), jnp.float32)

        @pl.when(j == 0)
        def _():
            clear(0, 2, 8, 88)

        @pl.when(j == flows - 1)
        def _():
            clear(4, 6, 8, 88)

        @pl.when(gy == 0)
        def _():
            clear(0, 6, 8, 16)

        @pl.when(gy == n_gy - 1)
        def _():
            clear(0, 6, 80, 88)

        pl.semaphore_wait(barrier, total)
        load.wait()

        def exchange(e, buf, wide, corners):
            view = lambda c, r: buf.at[:, pl.ds(*c), pl.ds(*r), :]
            sends, recvs = halo(e, view, 2, 2, wide, neighbour, exists, corners)
            run(sends)
            arrive(recvs)
            return sends

        pending = exchange(0, fb, 2, True)

        def valid(x, t):
            ok = inside(j * 2 + x - 2, 2 * flows)
            if t == 1:
                ok = ok & (gy > 0)
            if t == 10:
                ok = ok & (gy < n_gy - 1)
            return ok

        def near(src, f, x, r):
            return (src[f, x - 1, pl.ds(r, 8), :], src[f, x + 1, pl.ds(r, 8), :],
                    src[f, x, pl.ds(r - 1, 8), :], src[f, x, pl.ds(r + 1, 8), :])

        def first_sweep(dst, cols, tiles):
            def body(x, _):
                for t in tiles:
                    r = 8 * t
                    div = None
                    for f in range(3):
                        c = fb[f, x, pl.ds(r, 8), :]
                        we, ea, so, no = near(fb, f, x, r)
                        be = below(c)
                        total = ((we + ea) + (so + no)) + (be + above(c))
                        dst[f, x, pl.ds(r, 8), :] = jnp.where(valid(x, t), (1.2 * C) * c + CC * total, 0.0)
                        part = c - (we, so, be)[f]
                        div = part if div is None else div + part
                    dst[3, x, pl.ds(r, 8), :] = jnp.where(valid(x, t), (-0.5 * C) * div, 0.0)
                return 0
            loop(cols[0], cols[1], body, 0)

        def sweep(src, put, cols, tiles, masked):
            def body(x, _):
                for t in tiles:
                    r = 8 * t
                    p = src[3, x, pl.ds(r, 8), :]
                    toward = (src[3, x + 1, pl.ds(r, 8), :], src[3, x, pl.ds(r + 1, 8), :], above(p))
                    div = None
                    for f in range(3):
                        c = src[f, x, pl.ds(r, 8), :]
                        we, ea, so, no = near(src, f, x, r)
                        be = below(c)
                        total = ((we + ea) + (so + no)) + (be + above(c))
                        total = total + (fb[f, x, pl.ds(r, 8), :] - (toward[f] - p))
                        new = 0.2 * c + C * total
                        put(f, x, r, jnp.where(valid(x, t), new, 0.0) if masked else new)
                        part = c - (we, so, be)[f]
                        div = part if div is None else div + part
                    new = p - 0.5 * div
                    put(3, x, r, jnp.where(valid(x, t), new, 0.0) if masked else new)
                return 0
            loop(cols[0], cols[1], body, 0)

        def into(buf):
            def put(f, x, r, value):
                buf[f, x, pl.ds(r, 8), :] = value
            return put

        def final(f, x, r, value):
            if f < 3:
                out[f, x - 2, pl.ds(r - 16, 8), :] = value

        first_sweep(tmp, (1, 5), WIDE)
        sweep(tmp, into(e2), (2, 4), OWN, False)
        pending += exchange(1, e2, 1, False)
        sweep(e2, into(e3), (2, 4), OWN, False)

        view = lambda c, r: e3.at[:, pl.ds(*c), pl.ds(*r), :]
        sends3, recvs3 = halo(2, view, 2, 2, 2, neighbour, exists, True)
        run(sends3)
        plane = jnp.concatenate([e3[3, 2, 16:80, :], e3[3, 3, 16:80, :]], axis=0)
        spb[8] = plane.T[0:1, :]
        tells = []
        for dm, dy, ok, ident in beds:
            for r in range(3):
                slot = r + 2 - 3 * dm
                if 0 <= slot < 7:
                    tells.append((ok & (r_of == r), remote(spb.at[8], surf.at[1 - dy, slot], sus.at[1 - dy, slot],
                                                           sur.at[1 - dy, slot], ident)))
        run(tells)
        arrive(recvs3)
        pending += sends3 + tells
        sweep(e3, into(tmp), (1, 5), WIDE, True)
        sweep(tmp, into(e4), (2, 4), OWN, False)
        pending += exchange(3, e4, 2, True)
        sweep(e4, into(tmp), (1, 5), WIDE, True)
        sweep(tmp, final, (2, 4), OWN, False)

        for dm, dy, ok, ident in beds:
            @pl.when(ok)
            def _(dm=dm, dy=dy, ident=ident):
                remote(infs.at[8:11], infl.at[1 + dy, dm + 1], ins.at[0], inr.at[1 + dy, dm + 1], ident).wait_recv()
        even = lax.rem(sub, 2) == 0
        rows = []
        for s in range(3):
            parts = []
            for o in range(-2, 3):
                pick = [jnp.broadcast_to(infl[s, (r + o + 3) // 3, (r + o + 3) % 3], (8, 128)) for r in range(3)]
                parts.append(jnp.where(r_of == 0, pick[0], jnp.where(r_of == 1, pick[1], pick[2])))
            a = parts[0]
            for k in range(1, 5):
                a = jnp.where(sub >= 2 * k - 1, parts[k], a)
            rows.append((pltpu.roll(a, 32, 1), pltpu.roll(a, 96, 1)))
        middle = jnp.where(even, rows[1][1], rows[1][0])
        south = jnp.where(even, rows[0][0], rows[0][1])
        north = jnp.where(even, rows[2][0], rows[2][1])
        column = j * 2 - 3 + sub
        live = (column >= 0) & (column < 2 * flows)
        live = live & ((lane >= 32) | (gy > 0)) & ((lane < 96) | (gy < n_gy - 1))
        inflow = jnp.where(lane < 32, south, jnp.where(lane < 96, middle, north))
        inflow = jnp.where(live, inflow, 0.0)

        def plus(a, b):
            return b if a is None else (a if b is None else a + b)

        def minus(a, b):
            return a if b is None else (-b if a is None else a - b)

        def side(a, k):
            if a is None:
                return None
            return (pltpu.roll(a, 1, 0), pltpu.roll(a, 7, 0), pltpu.roll(a, 1, 1), pltpu.roll(a, 127, 1))[k]

        fields = [[None] * 6 for _ in range(4)]
        for step in range(4):
            new = [[None] * 6 for _ in range(4)]
            for z in range(step + 1):
                div = None
                for f in range(3):
                    c = fields[f][z]
                    if z > 0:
                        be = fields[f][z - 1]
                    else:
                        be = inflow if f == 2 else None
                    sides = [side(c, k) for k in range(4)]
                    total = plus(be, fields[f][z + 1])
                    for k in range(4):
                        total = plus(total, sides[k])
                    p = fields[3][z]
                    ahead = (side(p, 1), side(p, 3), fields[3][z + 1])[f]
                    total = plus(minus(total, ahead), p)
                    value = None if total is None else C * total
                    if c is not None:
                        value = plus(value, 0.2 * c)
                    new[f][z] = value
                    div = plus(div, minus(c, (sides[0], sides[2], be)[f]))
                if step < 3:
                    value = fields[3][z]
                    if div is not None:
                        value = minus(value, 0.5 * div)
                    new[3][z] = value
            for f in range(4):
                for z in range(step + 1):
                    if new[f][z] is not None:
                        new[f][z] = jnp.where(live, new[f][z], 0.0)
            fields = new
        stack = []
        for f in range(3):
            for c in range(2):
                acc = jnp.zeros((8, 128), jnp.float32)
                for z in range(4):
                    if fields[f][z] is not None:
                        acc = jnp.where(sub == z, pltpu.roll(fields[f][z], (z - 3 - c) % 8, 0), acc)
                stack.append(acc)
        stack.append(jnp.zeros((80, 128), jnp.float32))
        mt[...] = jnp.concatenate(stack, axis=0).T
        for t in range(8):
            turn = mt[32 + 8 * t:40 + 8 * t, :]
            for f in range(3):
                for c in range(2):
                    add = pltpu.roll(turn, (128 - 8 * (2 * f + c)) % 128, 1)
                    out[f, c, 8 * t:8 * t + 8, :] += jnp.where(lane < 8, add, 0.0)
        drain(pending)

    @pl.when(is_bed)
    def _():
        surf[...] = jnp.zeros_like(surf)
        loads = [pltpu.make_async_copy(perm, kb.at[0, 4:10, 16:80, :], lsem.at[0])]
        for c in range(3):
            loads.append(pltpu.make_async_copy(drive.at[c], kb.at[1, 4 + 2 * c:6 + 2 * c, 16:80, :], lsem.at[1 + c]))
        for cp in loads:
            cp.start()

        def neighbour(dx, dy):
            return (n_grp - 1, held(gx + dx, n_gx), held(gy + dy, n_gy))

        def exists(dx, dy):
            return inside(gx + dx, n_gx) & inside(gy + dy, n_gy)

        always = grp >= 0
        over_x = [(d, (n_grp - 1, lax.rem(gx + d, n_gx), gy)) for d in range(1, n_gx)]
        over_y = [(d, (n_grp - 1, gx, lax.rem(gy + d, n_gy))) for d in range(1, n_gy)]
        mates = []
        for k in range(7):
            flow = 3 * gx - 2 + k
            for dy in (-1, 0, 1):
                a, b = at(flow)
                mates.append((k, dy, inside(flow, flows) & inside(gy + dy, n_gy), (a, b, held(gy + dy, n_gy))))
        total = greet([(exists(dx, dy), neighbour(dx, dy)) for dx, dy in dirs]
                      + [(always, ident) for _, ident in over_x + over_y]
                      + [(ok, ident) for _, _, ok, ident in mates])

        def clear(c0, c1, r0, r1):
            kb[:, c0:c1, r0:r1, :] = jnp.zeros((2, c1 - c0, r1 - r0, 128), jnp.float32)

        @pl.when(gx == 0)
        def _():
            clear(0, 4, 8, 88)

        @pl.when(gx == n_gx - 1)
        def _():
            clear(10, 14, 8, 88)

        @pl.when(gy == 0)
        def _():
            clear(0, 14, 8, 16)

        @pl.when(gy == n_gy - 1)
        def _():
            clear(0, 14, 80, 88)

        pl.semaphore_wait(barrier, total)
        for cp in loads:
            cp.wait()
        view = lambda c, r: kb.at[:, pl.ds(*c), pl.ds(*r), :]
        pending, recvs = halo(4, view, 4, 6, 4, neighbour, exists, True)
        run(pending)
        arrive(recvs)

        def weight(x, _):
            open_x = gx >= 0
            if x == 3:
                open_x = gx > 0
            if x == 9:
                open_x = gx < n_gx - 1
            for t in WIDE:
                r = 8 * t
                k = kb[0, x, pl.ds(r, 8), :]
                w[0, x, pl.ds(r, 8), :] = jnp.where(open_x, (k + kb[0, x + 1, pl.ds(r, 8), :]) * (0.5 * SCALE), 0.0)
                wy = (k + kb[0, x, pl.ds(r + 1, 8), :]) * (0.5 * SCALE)
                if t == 1:
                    wy = jnp.where((gy == 0) & (sub == 7), 0.0, wy)
                if t == 9:
                    wy = jnp.where((gy == n_gy - 1) & (sub == 7), 0.0, wy)
                w[1, x, pl.ds(r, 8), :] = wy
                up = pltpu.roll(k, 127, 1)
                w[2, x, pl.ds(r, 8), :] = jnp.where(l127, k * SCALE, (k + up) * (0.5 * SCALE))
            return 0

        loop(0, 13, weight, 0)

        def image(src, x, t):
            r = 8 * t
            f = src(x, r)
            ge = w[0, x, pl.ds(r, 8), :] * (f - src(x + 1, r))
            gw = w[0, x - 1, pl.ds(r, 8), :] * (f - src(x - 1, r))
            gn = w[1, x, pl.ds(r, 8), :] * (f - src(x, r + 1))
            gs = w[1, x, pl.ds(r - 1, 8), :] * (f - src(x, r - 1))
            gz = w[2, x, pl.ds(r, 8), :] * (f - above(f))
            return ((ge + gw) + (gn + gs)) + (gz - below(gz))

        def reader(ref):
            return lambda x, r: ref[x, pl.ds(r, 8), :]

        r1, r2, r3 = reader(v1), reader(v2), reader(v3)

        def powers(src):
            for here, there, lo, hi in ((src, v1, 1, 13), (r1, v2, 2, 12), (r2, v3, 3, 11)):
                def body(x, _, here=here, there=there):
                    for t in WIDE:
                        there[x, pl.ds(8 * t, 8), :] = image(here, x, t)
                    return 0
                loop(lo, hi, body, 0)

            def body(x, acc):
                acc = list(acc)
                for t in OWN:
                    v = [get(x, 8 * t) for get in (src, r1, r2, r3)] + [image(r3, x, t)]
                    for i in range(8):
                        s, e = two_sum(acc[2 * i], v[i // 2] * v[(i + 1) // 2])
                        acc[2 * i] = s
                        acc[2 * i + 1] = acc[2 * i + 1] + e
                return tuple(acc)
            acc = loop(4, 10, body, tuple(jnp.zeros((8, 128), jnp.float32) for _ in range(16)))
            level = [(acc[2 * i], acc[2 * i + 1]) for i in range(8)]
            for d in (4, 2, 1):
                keep = (sub & d) == 0
                nxt = []
                for i in range(d):
                    a, b = level[i], level[i + d]
                    x = [jnp.where(keep, a[h], b[h]) for h in range(2)]
                    y = [jnp.where(keep, b[h], a[h]) for h in range(2)]
                    y = [jnp.where(keep, pltpu.roll(q, 8 - d, 0), pltpu.roll(q, d, 0)) for q in y]
                    s, e = two_sum(x[0], y[0])
                    nxt.append((s, e + (x[1] + y[1])))
                level = nxt
            return level[0]

        def spread_x(s, pair):
            ar1[s, 0, 0] = pair[0]
            ar1[s, 0, 1] = pair[1]
            cps = [(always, remote(ar1.at[s, 0], ar1.at[s, d], a1s.at[s, d], a1r.at[s, d], ident)) for d, ident in over_x]
            run(cps)
            return cps

        def spread_y(s, cps):
            arrive(cps)
            hi, lo = tree((ar1[s, d, 0], ar1[s, d, 1]) for d in range(n_gx))
            big = jnp.max(jnp.abs(hi), axis=1, keepdims=True) * 512.0
            top = (hi + big) - big
            th = jnp.sum(top, axis=1, keepdims=True)
            tl = jnp.sum((hi - top) + lo, axis=1, keepdims=True)
            th, tl = two_sum(th, tl)
            spot = jnp.where(lane == sub, th, jnp.where(lane == sub + 8, tl, 0.0))
            ar2[s, 8] = jnp.sum(spot, axis=0, keepdims=True)
            out_cps = [(always, remote(ar2.at[s, 8], ar2.at[s, 8 + d], a2s.at[s, d], a2r.at[s, d], ident)) for d, ident in over_y]
            run(out_cps)
            return out_cps

        def solve(s, cps):
            arrive(cps)
            hi, lo = tree((ar2[s, 8 + d], jnp.zeros((1, 128), jnp.float32)) for d in range(n_gy))
            hi = jnp.broadcast_to(hi, (8, 128))
            lo = jnp.broadcast_to(lo, (8, 128))
            th = jnp.sum(jnp.where(lane == sub, hi, 0.0), axis=1, keepdims=True)
            tl = jnp.sum(jnp.where(lane == sub, lo, jnp.where(lane == sub + 8, hi, 0.0)), axis=1, keepdims=True)
            th = jnp.broadcast_to(th, (8, 128))
            tl = jnp.broadcast_to(tl, (8, 128))
            mu = [quick(jnp.broadcast_to(th[i:i + 1], (8, 128)), jnp.broadcast_to(tl[i:i + 1], (8, 128))) for i in range(8)]
            return coefficients(mu)

        def source(x, r):
            return kb[1, x, pl.ds(r, 8), :]

        first_x = spread_x(0, powers(source))

        tiles = []
        for c in range(2):
            for t in OWN:
                acc = jnp.zeros((8, 128), jnp.float32)
                for q in range(3):
                    x = 4 + 2 * q + c
                    k = kb[0, x, pl.ds(8 * t, 8), :]
                    for i, get in enumerate((source, r1, r2, r3)):
                        at_lane = i * 8 + q
                        acc = jnp.where(lane == at_lane, pltpu.roll(k * get(x, 8 * t), at_lane + 1, 1), acc)
                tiles.append(acc)
        zt[...] = jnp.concatenate(tiles, axis=0).T[0:32, :]

        first_y = spread_y(0, first_x)

        for k, dy, ok, ident in mates:
            @pl.when(ok)
            def _(k=k, dy=dy, ident=ident):
                remote(spb.at[8], surf.at[1 + dy, k], sus.at[0, 0], sur.at[1 + dy, k], ident).wait_recv()
        rows = []
        for s in range(3):
            a = jnp.zeros((8, 128), jnp.float32)
            for k in range(7):
                a = jnp.where(sub == k, jnp.broadcast_to(surf[s, k], (8, 128)), a)
            rows.append(a)
        rows.append(jnp.zeros((104, 128), jnp.float32))
        mt[...] = jnp.concatenate(rows, axis=0).T
        for k in range(7):
            for c in range(2):
                x = 2 * k + c
                for t in WIDE:
                    if t == 1:
                        r, at_lane = c * 64 + 56, k
                    elif t == 10:
                        r, at_lane = c * 64, 16 + k
                    else:
                        r, at_lane = c * 64 + 8 * (t - 2), 8 + k
                    p = pltpu.roll(mt[r:r + 8, :], 127 - at_lane, 1)
                    k8 = kb[0, x, pl.ds(8 * t, 8), :]
                    b2[x, pl.ds(8 * t, 8), :] = kb[1, x, pl.ds(8 * t, 8), :] + jnp.where(l127, k8 * (0.5 * p), 0.0)

        second_x = spread_x(1, powers(reader(b2)))
        second_y = spread_y(1, second_x)
        c1 = solve(0, first_y)
        flow_in = c1[0] * zt[0:8, :]
        for i in range(1, 4):
            flow_in = flow_in + c1[i] * zt[8 * i:8 * i + 8, :]
        for q in range(3):
            infs[8 + q] = flow_in[q:q + 1, :]
        tells = []
        for k, dy, ok, ident in mates:
            dm = (1, 1, 0, 0, 0, -1, -1)[k]
            tells.append((ok, remote(infs.at[8:11], infl.at[1 - dy, dm + 1], ins.at[k * 3 + dy + 1], inr.at[1 - dy, dm + 1], ident)))
        run(tells)
        c2 = solve(1, second_y)

        for x in range(4, 10):
            for t in OWN:
                rows8 = pl.ds(8 * t, 8)
                total = (c2[0] * b2[x, rows8, :] + c2[1] * v1[x, rows8, :]) + (c2[2] * v2[x, rows8, :] + c2[3] * v3[x, rows8, :])
                out[(x - 4) // 2, x % 2, pl.ds(8 * t - 16, 8), :] = total
        drain(pending + first_x + first_y + second_x + second_y + tells)


def solution(mesh):
    n_grp, n_gx, n_gy = mesh.shape["grp"], mesh.shape["gx"], mesh.shape["gy"]

    def per_device(drive, permeability):
        vmem = lambda *shape: pltpu.VMEM(shape, jnp.float32)
        dma = lambda *shape: pltpu.SemaphoreType.DMA(shape)
        return pl.pallas_call(
            functools.partial(kernel, n_grp, n_gx, n_gy),
            out_shape=jax.ShapeDtypeStruct(drive.shape, jnp.float32),
            in_specs=[pl.BlockSpec(memory_space=pl.ANY)] * 2,
            out_specs=pl.BlockSpec(memory_space=pltpu.VMEM),
            scratch_shapes=[
                vmem(3, 6, ROWS, 128), vmem(4, 6, ROWS, 128), vmem(4, 6, ROWS, 128),
                vmem(4, 6, ROWS, 128), vmem(4, 6, ROWS, 128),
                vmem(2, 14, ROWS, 128), vmem(3, 14, ROWS, 128),
                vmem(14, ROWS, 128), vmem(14, ROWS, 128), vmem(14, ROWS, 128), vmem(14, ROWS, 128),
                vmem(128, 128), vmem(32, 128),
                vmem(4, 8, 1, 128), vmem(24, 1, 128), vmem(4, 3, 3, 1, 128), vmem(24, 1, 128),
                vmem(2, 8, 2, 8, 128), vmem(2, 32, 1, 128),
                dma(4), dma(5, 9), dma(5, 9), dma(2, 8), dma(2, 8), dma(2, 16), dma(2, 16),
                dma(3, 7), dma(3, 7), dma(21), dma(3, 3),
            ],
            compiler_params=pltpu.CompilerParams(collective_id=0, has_side_effects=True, vmem_limit_bytes=40 * 1024 * 1024),
            name="coupling",
        )(drive, permeability)

    return jax.shard_map(
        per_device,
        mesh=mesh,
        in_specs=(P(None, ("grp", "gx"), "gy", None), P("gx", "gy", None)),
        out_specs=P(None, ("grp", "gx"), "gy", None),
        check_vma=False,
    )
```

```python
import functools
import jax
import jax.numpy as jnp
from jax import lax
from jax.experimental import pallas as pl
from jax.experimental.pallas import tpu as pltpu
from jax.sharding import PartitionSpec as P

MESH = pl.DeviceIdType.MESH
C = 0.8 / 6.0
CC = (0.8 / 6.0) * (0.8 / 6.0)
SCALE = 1.0 / 16.0
ROWS = 96
OWN = range(2, 10)
WIDE = range(1, 11)


def loop(lo, hi, body, carry):
    for x in range(lo, hi):
        carry = body(x, carry)
    return carry


def two_sum(a, b):
    s = a + b
    bb = s - a
    return s, (a - (s - bb)) + (b - bb)


def quick(a, b):
    s = a + b
    return s, b - (s - a)


def halves(a):
    t = a * 4097.0
    hi = t - (t - a)
    return hi, a - hi


def two_prod(a, b):
    p = a * b
    ah, al = halves(a)
    bh, bl = halves(b)
    return p, ((ah * bh - p) + ah * bl + al * bh) + al * bl


def dadd(a, b):
    s, e = two_sum(a[0], b[0])
    return quick(s, e + (a[1] + b[1]))


def dsub(a, b):
    return dadd(a, (-b[0], -b[1]))


def dmul(a, b):
    p, e = two_prod(a[0], b[0])
    return quick(p, e + (a[0] * b[1] + a[1] * b[0]))


def drecip(a):
    r = 1.0 / a[0]
    p, pe = two_prod(r, a[0])
    e = ((1.0 - p) - pe) - r * a[1]
    return quick(r, r * e)


def tree(pairs):
    pairs = list(pairs)
    while len(pairs) > 1:
        nxt = []
        for i in range(0, len(pairs) - 1, 2):
            (ah, al), (bh, bl) = pairs[i], pairs[i + 1]
            s, e = two_sum(ah, bh)
            nxt.append((s, e + (al + bl)))
        if len(pairs) % 2:
            nxt.append(pairs[-1])
        pairs = nxt
    return pairs[0]


def coefficients(mu):
    n = 4
    m = [[mu[i + j + 1] for j in range(n)] for i in range(n)]
    y = [mu[i] for i in range(n)]
    low = [[None] * n for _ in range(n)]
    inv = [None] * n
    for k in range(n):
        good = m[k][k][0] > 1e-12 * mu[2 * k + 1][0]
        safe = jnp.where(good, m[k][k][0], 1.0)
        rh, rl = drecip((safe, m[k][k][1]))
        inv[k] = (jnp.where(good, rh, 0.0), jnp.where(good, rl, 0.0))
        for i in range(k + 1, n):
            low[i][k] = dmul(m[i][k], inv[k])
        for i in range(k + 1, n):
            for j in range(k + 1, i + 1):
                m[i][j] = dsub(m[i][j], dmul(low[i][k], m[j][k]))
                m[j][i] = m[i][j]
            y[i] = dsub(y[i], dmul(low[i][k], y[k]))
    c = [None] * n
    for k in range(n - 1, -1, -1):
        s = dmul(y[k], inv[k])
        for i in range(k + 1, n):
            s = dsub(s, dmul(low[i][k], c[i]))
        c[k] = s
    return [v[0] * SCALE for v in c]


def kernel(n_grp, n_gx, n_gy, drive, perm, out, fb, e2, e3, e4, tmp, kb, w, v1, v2, v3, b2, mt, zt,
           surf, spb, infl, infs, ar1, ar2, nb, nbs,
           lsem, hs, hr, a1s, a1r, a2s, a2r, sus, sur, ins, inr, ns, nr, tok, ready):
    grp = lax.axis_index("grp")
    gx = lax.axis_index("gx")
    gy = lax.axis_index("gy")
    flows = (n_grp - 1) * n_gx
    is_bed = grp == n_grp - 1
    j = grp * n_gx + gx
    m_of = lax.div(j, 3)
    r_of = j - 3 * m_of
    lane = lax.broadcasted_iota(jnp.int32, (8, 128), 1)
    sub = lax.broadcasted_iota(jnp.int32, (8, 128), 0)
    l0 = lane == 0
    l127 = lane == 127

    def inside(i, n):
        return (i >= 0) & (i < n)

    def held(i, n):
        return jnp.minimum(jnp.maximum(i, 0), n - 1)

    def at(flow):
        flow = held(flow, flows)
        return (lax.div(flow, n_gx), lax.rem(flow, n_gx))

    def below(f):
        return jnp.where(l0, 0.0, pltpu.roll(f, 1, 1))

    def above(f):
        return jnp.where(l127, 0.0, pltpu.roll(f, 127, 1))

    barrier = pltpu.get_barrier_semaphore()
    dirs = [(dx, dy) for dx in (-1, 0, 1) for dy in (-1, 0, 1) if (dx, dy) != (0, 0)]

    def greet(partners):
        total = jnp.int32(0)
        for ok, ident in partners:
            @pl.when(ok)
            def _(ident=ident):
                pl.semaphore_signal(barrier, inc=1, device_id=ident, device_id_type=MESH)
            total = total + ok.astype(jnp.int32)
        return total

    def run(copies):
        for ok, cp in copies:
            @pl.when(ok)
            def _(cp=cp):
                cp.start()

    def arrive(copies):
        for ok, cp in copies:
            @pl.when(ok)
            def _(cp=cp):
                cp.wait_recv()

    def drain(copies):
        for ok, cp in copies:
            @pl.when(ok)
            def _(cp=cp):
                cp.wait_send()

    def remote(src, dst, s, r, ident):
        return pltpu.make_async_remote_copy(src_ref=src, dst_ref=dst, send_sem=s, recv_sem=r,
                                            device_id=ident, device_id_type=MESH)

    def halo(e, view, first, width, wide, neighbour, exists, corners):
        sends, recvs = [], []
        for dx, dy in dirs:
            if not corners and dx != 0 and dy != 0:
                continue
            if dx == 0:
                sc, dc = (first, width), (first, width)
            elif dx == 1:
                sc, dc = (first + width - wide, wide), (first - wide, wide)
            else:
                sc, dc = (first, wide), (first + width, wide)
            if dy == 0:
                sr, dr = (16, 64), (16, 64)
            elif dy == 1:
                sr, dr = (72, 8), (8, 8)
            else:
                sr, dr = (16, 8), (80, 8)
            d = (dx + 1) * 3 + dy + 1
            cp = remote(view(sc, sr), view(dc, dr), hs.at[e, d], hr.at[e, d], neighbour(dx, dy))
            sends.append((exists(dx, dy), cp))
            recvs.append((exists(-dx, -dy), remote(view(sc, sr), view(dc, dr), hs.at[e, d], hr.at[e, d],
                                                   neighbour(-dx, -dy))))
        return sends, recvs

    @pl.when(jnp.logical_not(is_bed))
    def _():
        infl[...] = jnp.zeros_like(infl)
        nb[...] = jnp.zeros_like(nb)
        load = pltpu.make_async_copy(drive, fb.at[:, 2:4, 16:80, :], lsem.at[0])
        load.start()

        def neighbour(dx, dy):
            a, b = at(j + dx)
            return (a, b, held(gy + dy, n_gy))

        def exists(dx, dy):
            return inside(j + dx, flows) & inside(gy + dy, n_gy)

        beds = []
        for dm in (-1, 0, 1):
            for dy in (-1, 0, 1):
                ok = inside(m_of + dm, n_gx) & inside(gy + dy, n_gy)
                if dm == -1:
                    ok = ok & (r_of <= 1)
                if dm == 1:
                    ok = ok & (r_of >= 1)
                beds.append((dm, dy, ok, (n_grp - 1, held(m_of + dm, n_gx), held(gy + dy, n_gy))))

        around = [(o, dy) for o in range(-2, 3) for dy in (-1, 0, 1) if (o, dy) != (0, 0)]
        total = greet([(exists(o, dy), neighbour(o, dy)) for o, dy in around])
        greet([(ok, ident) for _, _, ok, ident in beds])

        def clear(c0, c1, r0, r1):
            for buf in (fb, e2, e3, e4):
                buf[:, c0:c1, r0:r1, :] = jnp.zeros((buf.shape[0], c1 - c0, r1 - r0, 128), jnp.float32)

        @pl.when(j == 0)
        def _():
            clear(0, 2, 8, 88)

        @pl.when(j == flows - 1)
        def _():
            clear(4, 6, 8, 88)

        @pl.when(gy == 0)
        def _():
            clear(0, 6, 8, 16)

        @pl.when(gy == n_gy - 1)
        def _():
            clear(0, 6, 80, 88)

        load.wait()

        tiles = []
        for c in range(2):
            for t in OWN:
                acc = fb[0, 2 + c, 8 * t:8 * t + 8, :]
                for f in (1, 2):
                    acc = jnp.where(lane >= 3 * f, pltpu.roll(fb[f, 2 + c, 8 * t:8 * t + 8, :], 3 * f, 1), acc)
                tiles.append(acc)
        turned = jnp.concatenate(tiles, axis=0).T
        for q in range(9):
            nbs[8 + q] = turned[q:q + 1, :]
        pl.semaphore_wait(barrier, total)
        low_out, low_in = [], []
        for o, dy in around:
            low_out.append((exists(o, dy), remote(nbs.at[8:17], nb.at[1 - dy, 2 - o], ns.at[dy + 1, o + 2],
                                                  nr.at[1 - dy, 2 - o], neighbour(o, dy))))
            low_in.append((exists(o, dy), remote(nbs.at[8:17], nb.at[1 + dy, 2 + o], ns.at[dy + 1, o + 2],
                                                 nr.at[1 + dy, 2 + o], neighbour(o, dy))))
        run(low_out)

        def begin(e, buf, wide, corners):
            view = lambda c, r: buf.at[:, pl.ds(*c), pl.ds(*r), :]
            sends, recvs = halo(e, view, 2, 2, wide, neighbour, exists, corners)
            run(sends)
            return sends, recvs

        def exchange(e, buf, wide, corners):
            sends, recvs = begin(e, buf, wide, corners)
            arrive(recvs)
            return sends

        pending, recvs0 = begin(0, fb, 2, True)
        pending = pending + low_out

        even = lax.rem(sub, 2) == 0
        column = j * 2 - 3 + sub
        live = (column >= 0) & (column < 2 * flows)
        live = live & ((lane >= 32) | (gy > 0)) & ((lane < 96) | (gy < n_gy - 1))

        def assemble(row):
            rows = []
            for i in range(3):
                a = row(i, -2)
                for o in range(-1, 3):
                    a = jnp.where(sub >= 2 * o + 3, row(i, o), a)
                rows.append((pltpu.roll(a, 32, 1), pltpu.roll(a, 96, 1)))
            middle = jnp.where(even, rows[1][1], rows[1][0])
            south = jnp.where(even, rows[0][0], rows[0][1])
            north = jnp.where(even, rows[2][0], rows[2][1])
            whole = jnp.where(lane < 32, south, jnp.where(lane < 96, middle, north))
            return jnp.where(live, whole, 0.0)

        def plus(a, b):
            return b if a is None else (a if b is None else a + b)

        def minus(a, b):
            return a if b is None else (-b if a is None else a - b)

        def side(a, k):
            if a is None:
                return None
            return (pltpu.roll(a, 1, 0), pltpu.roll(a, 7, 0), pltpu.roll(a, 1, 1), pltpu.roll(a, 127, 1))[k]

        def evolve(fields, inflow, force, n_velocity, n_pressure):
            new = [[None] * 6 for _ in range(4)]
            for z in range(max(n_velocity, n_pressure)):
                div = None
                for f in range(3):
                    c = fields[f][z]
                    if z > 0:
                        be = fields[f][z - 1]
                    else:
                        be = inflow if f == 2 else None
                    sides = [side(c, k) for k in range(4)]
                    if z < n_velocity:
                        total = plus(plus(be, fields[f][z + 1]), force[f][z])
                        for k in range(4):
                            total = plus(total, sides[k])
                        p = fields[3][z]
                        ahead = (side(p, 1), side(p, 3), fields[3][z + 1])[f]
                        total = plus(minus(total, ahead), p)
                        value = None if total is None else C * total
                        if c is not None:
                            value = plus(value, 0.2 * c)
                        if value is not None:
                            new[f][z] = jnp.where(live, value, 0.0)
                    div = plus(div, minus(c, (sides[0], sides[2], be)[f]))
                if z < n_pressure:
                    value = fields[3][z]
                    if div is not None:
                        value = minus(value, 0.5 * div)
                    if value is not None:
                        new[3][z] = jnp.where(live, value, 0.0)
            return new

        nothing = [[None] * 6 for _ in range(4)]
        arrive(low_in)
        force = [[None] * 6 for _ in range(3)]
        for f in range(3):
            for z in range(3):
                q = 3 * f + z

                def row(i, o, q=q):
                    one = nbs[8 + q] if (i, o) == (1, 0) else nb[i, o + 2, q]
                    return jnp.broadcast_to(one, (8, 128))
                force[f][z] = assemble(row)
        low = evolve(nothing, None, force, 3, 0)
        low = evolve(low, None, force, 2, 2)
        low = evolve(low, None, force, 1, 1)
        low = evolve(low, None, force, 0, 1)[3][0]
        spb[8] = jnp.where(lane[0:1] < 64, pltpu.roll(low, 96, 1)[3:4], pltpu.roll(low, 32, 1)[4:5])
        tells = []
        for dm, dy, ok, ident in beds:
            @pl.when(ok)
            def _(dm=dm, dy=dy):
                pl.semaphore_wait(ready.at[1 + dy, dm + 1], 1)
            for r in range(3):
                slot = r + 2 - 3 * dm
                if 0 <= slot < 7:
                    tells.append((ok & (r_of == r), remote(spb.at[8], surf.at[1 - dy, slot], sus.at[1 - dy, slot],
                                                           sur.at[1 - dy, slot], ident)))
        run(tells)
        pending = pending + tells
        arrive(recvs0)

        def valid(x, t):
            ok = inside(j * 2 + x - 2, 2 * flows)
            if t == 1:
                ok = ok & (gy > 0)
            if t == 10:
                ok = ok & (gy < n_gy - 1)
            return ok

        def near(src, f, x, r):
            return (src[f, x - 1, pl.ds(r, 8), :], src[f, x + 1, pl.ds(r, 8), :],
                    src[f, x, pl.ds(r - 1, 8), :], src[f, x, pl.ds(r + 1, 8), :])

        def first_sweep(dst, cols, tiles):
            def body(x, _):
                for t in tiles:
                    r = 8 * t
                    div = None
                    for f in range(3):
                        c = fb[f, x, pl.ds(r, 8), :]
                        we, ea, so, no = near(fb, f, x, r)
                        be = below(c)
                        total = ((we + ea) + (so + no)) + (be + above(c))
                        dst[f, x, pl.ds(r, 8), :] = jnp.where(valid(x, t), (1.2 * C) * c + CC * total, 0.0)
                        part = c - (we, so, be)[f]
                        div = part if div is None else div + part
                    dst[3, x, pl.ds(r, 8), :] = jnp.where(valid(x, t), (-0.5 * C) * div, 0.0)
                return 0
            loop(cols[0], cols[1], body, 0)

        def sweep(src, put, cols, tiles, masked):
            def body(x, _):
                for t in tiles:
                    r = 8 * t
                    p = src[3, x, pl.ds(r, 8), :]
                    toward = (src[3, x + 1, pl.ds(r, 8), :], src[3, x, pl.ds(r + 1, 8), :], above(p))
                    div = None
                    for f in range(3):
                        c = src[f, x, pl.ds(r, 8), :]
                        we, ea, so, no = near(src, f, x, r)
                        be = below(c)
                        total = ((we + ea) + (so + no)) + (be + above(c))
                        total = total + (fb[f, x, pl.ds(r, 8), :] - (toward[f] - p))
                        new = 0.2 * c + C * total
                        put(f, x, r, jnp.where(valid(x, t), new, 0.0) if masked else new)
                        part = c - (we, so, be)[f]
                        div = part if div is None else div + part
                    new = p - 0.5 * div
                    put(3, x, r, jnp.where(valid(x, t), new, 0.0) if masked else new)
                return 0
            loop(cols[0], cols[1], body, 0)

        def into(buf):
            def put(f, x, r, value):
                buf[f, x, pl.ds(r, 8), :] = value
            return put

        def final(f, x, r, value):
            if f < 3:
                out[f, x - 2, pl.ds(r - 16, 8), :] = value

        first_sweep(tmp, (1, 5), WIDE)
        sweep(tmp, into(e2), (2, 4), OWN, False)
        pending += exchange(1, e2, 1, False)
        sweep(e2, into(e3), (2, 4), OWN, False)

        pending += exchange(2, e3, 2, True)
        sweep(e3, into(tmp), (1, 5), WIDE, True)
        sweep(tmp, into(e4), (2, 4), OWN, False)
        pending += exchange(3, e4, 2, True)
        sweep(e4, into(tmp), (1, 5), WIDE, True)
        sweep(tmp, final, (2, 4), OWN, False)

        for dm, dy, ok, ident in beds:
            @pl.when(ok)
            def _(dm=dm, dy=dy, ident=ident):
                remote(infs.at[8:11], infl.at[1 + dy, dm + 1], ins.at[0], inr.at[1 + dy, dm + 1], ident).wait_recv()

        def row(i, o):
            pick = [jnp.broadcast_to(infl[i, (r + o + 3) // 3, (r + o + 3) % 3], (8, 128)) for r in range(3)]
            return jnp.where(r_of == 0, pick[0], jnp.where(r_of == 1, pick[1], pick[2]))

        inflow = assemble(row)
        fields = nothing
        for step in range(4):
            fields = evolve(fields, inflow, nothing, step + 1, step + 1 if step < 3 else 0)
        stack = []
        for f in range(3):
            for c in range(2):
                acc = jnp.zeros((8, 128), jnp.float32)
                for z in range(4):
                    if fields[f][z] is not None:
                        acc = jnp.where(sub == z, pltpu.roll(fields[f][z], (z - 3 - c) % 8, 0), acc)
                stack.append(acc)
        stack.append(jnp.zeros((80, 128), jnp.float32))
        mt[...] = jnp.concatenate(stack, axis=0).T
        for t in range(8):
            turn = mt[32 + 8 * t:40 + 8 * t, :]
            for f in range(3):
                for c in range(2):
                    add = pltpu.roll(turn, (128 - 8 * (2 * f + c)) % 128, 1)
                    out[f, c, 8 * t:8 * t + 8, :] += jnp.where(lane < 8, add, 0.0)
        drain(pending)

    @pl.when(is_bed)
    def _():
        surf[...] = jnp.zeros_like(surf)
        loads = [pltpu.make_async_copy(perm, kb.at[0, 4:10, 16:80, :], lsem.at[0])]
        for c in range(3):
            loads.append(pltpu.make_async_copy(drive.at[c], kb.at[1, 4 + 2 * c:6 + 2 * c, 16:80, :], lsem.at[1 + c]))
        for cp in loads:
            cp.start()

        def neighbour(dx, dy):
            return (n_grp - 1, held(gx + dx, n_gx), held(gy + dy, n_gy))

        def exists(dx, dy):
            return inside(gx + dx, n_gx) & inside(gy + dy, n_gy)

        always = grp >= 0

        def ring(d):
            return (n_grp - 1, gx, lax.rem(gy + d + n_gy, n_gy))

        over_x = [(d, (n_grp - 1, lax.rem(gx + d, n_gx), gy)) for d in range(1, n_gx)]
        over_y = [(d, (n_grp - 1, gx, lax.rem(gy + d, n_gy))) for d in range(1, n_gy)]
        mates = []
        for k in range(7):
            flow = 3 * gx - 2 + k
            for dy in (-1, 0, 1):
                a, b = at(flow)
                mates.append((k, dy, inside(flow, flows) & inside(gy + dy, n_gy), (a, b, held(gy + dy, n_gy))))
        total = greet([(exists(dx, dy), neighbour(dx, dy)) for dx, dy in dirs]
                      + [(always, ident) for _, ident in over_x]
                      + [(always, ring(d)) for d in (-1, 1)])
        for _, _, ok, _ in mates:
            total = total + ok.astype(jnp.int32)

        def clear(c0, c1, r0, r1):
            kb[:, c0:c1, r0:r1, :] = jnp.zeros((2, c1 - c0, r1 - r0, 128), jnp.float32)

        @pl.when(gx == 0)
        def _():
            clear(0, 4, 8, 88)

        @pl.when(gx == n_gx - 1)
        def _():
            clear(10, 14, 8, 88)

        @pl.when(gy == 0)
        def _():
            clear(0, 14, 8, 16)

        @pl.when(gy == n_gy - 1)
        def _():
            clear(0, 14, 80, 88)

        for cp in loads:
            cp.wait()
        pl.semaphore_wait(barrier, total)
        for d in (-1, 1):
            pl.semaphore_signal(tok.at[0, (d + 1) // 2], inc=1, device_id=ring(d), device_id_type=MESH)
        view = lambda c, r: kb.at[:, pl.ds(*c), pl.ds(*r), :]
        pending, recvs = halo(4, view, 4, 6, 4, neighbour, exists, True)
        run(pending)
        for k, dy, ok, ident in mates:
            @pl.when(ok)
            def _(k=k, dy=dy, ident=ident):
                pl.semaphore_signal(ready.at[1 - dy, (1, 1, 0, 0, 0, -1, -1)[k] + 1], inc=1, device_id=ident,
                                    device_id_type=MESH)
        for i, far in enumerate((2, 4, 0)):
            for h in range(2):
                pl.semaphore_wait(tok.at[i, h], 1)
            if far:
                for h in range(2):
                    pl.semaphore_signal(tok.at[i + 1, h], inc=1, device_id=ring((2 * h - 1) * far), device_id_type=MESH)
        arrive(recvs)

        def weight(x, _):
            open_x = gx >= 0
            if x == 3:
                open_x = gx > 0
            if x == 9:
                open_x = gx < n_gx - 1
            for t in WIDE:
                r = 8 * t
                k = kb[0, x, pl.ds(r, 8), :]
                w[0, x, pl.ds(r, 8), :] = jnp.where(open_x, (k + kb[0, x + 1, pl.ds(r, 8), :]) * (0.5 * SCALE), 0.0)
                wy = (k + kb[0, x, pl.ds(r + 1, 8), :]) * (0.5 * SCALE)
                if t == 1:
                    wy = jnp.where((gy == 0) & (sub == 7), 0.0, wy)
                if t == 9:
                    wy = jnp.where((gy == n_gy - 1) & (sub == 7), 0.0, wy)
                w[1, x, pl.ds(r, 8), :] = wy
                up = pltpu.roll(k, 127, 1)
                w[2, x, pl.ds(r, 8), :] = jnp.where(l127, k * SCALE, (k + up) * (0.5 * SCALE))
            return 0

        loop(0, 13, weight, 0)

        def image(src, x, t):
            r = 8 * t
            f = src(x, r)
            ge = w[0, x, pl.ds(r, 8), :] * (f - src(x + 1, r))
            gw = w[0, x - 1, pl.ds(r, 8), :] * (f - src(x - 1, r))
            gn = w[1, x, pl.ds(r, 8), :] * (f - src(x, r + 1))
            gs = w[1, x, pl.ds(r - 1, 8), :] * (f - src(x, r - 1))
            gz = w[2, x, pl.ds(r, 8), :] * (f - above(f))
            return ((ge + gw) + (gn + gs)) + (gz - below(gz))

        def reader(ref):
            return lambda x, r: ref[x, pl.ds(r, 8), :]

        r1, r2, r3 = reader(v1), reader(v2), reader(v3)

        def powers(src):
            for here, there, lo, hi in ((src, v1, 1, 13), (r1, v2, 2, 12), (r2, v3, 3, 11)):
                def body(x, _, here=here, there=there):
                    for t in WIDE:
                        there[x, pl.ds(8 * t, 8), :] = image(here, x, t)
                    return 0
                loop(lo, hi, body, 0)

            def body(x, acc):
                acc = list(acc)
                for t in OWN:
                    v = [get(x, 8 * t) for get in (src, r1, r2, r3)] + [image(r3, x, t)]
                    for i in range(8):
                        s, e = two_sum(acc[2 * i], v[i // 2] * v[(i + 1) // 2])
                        acc[2 * i] = s
                        acc[2 * i + 1] = acc[2 * i + 1] + e
                return tuple(acc)
            acc = loop(4, 10, body, tuple(jnp.zeros((8, 128), jnp.float32) for _ in range(16)))
            level = [(acc[2 * i], acc[2 * i + 1]) for i in range(8)]
            for d in (4, 2, 1):
                keep = (sub & d) == 0
                nxt = []
                for i in range(d):
                    a, b = level[i], level[i + d]
                    x = [jnp.where(keep, a[h], b[h]) for h in range(2)]
                    y = [jnp.where(keep, b[h], a[h]) for h in range(2)]
                    y = [jnp.where(keep, pltpu.roll(q, 8 - d, 0), pltpu.roll(q, d, 0)) for q in y]
                    s, e = two_sum(x[0], y[0])
                    nxt.append((s, e + (x[1] + y[1])))
                level = nxt
            return level[0]

        def spread_x(s, pair):
            ar1[s, 0, 0] = pair[0]
            ar1[s, 0, 1] = pair[1]
            cps = [(always, remote(ar1.at[s, 0], ar1.at[s, d], a1s.at[s, d], a1r.at[s, d], ident)) for d, ident in over_x]
            run(cps)
            return cps

        def spread_y(s, cps):
            arrive(cps)
            hi, lo = tree((ar1[s, d, 0], ar1[s, d, 1]) for d in range(n_gx))
            big = jnp.max(jnp.abs(hi), axis=1, keepdims=True) * 512.0
            top = (hi + big) - big
            th = jnp.sum(top, axis=1, keepdims=True)
            tl = jnp.sum((hi - top) + lo, axis=1, keepdims=True)
            th, tl = two_sum(th, tl)
            spot = jnp.where(lane == sub, th, jnp.where(lane == sub + 8, tl, 0.0))
            ar2[s, 8] = jnp.sum(spot, axis=0, keepdims=True)
            out_cps = [(always, remote(ar2.at[s, 8], ar2.at[s, 8 + d], a2s.at[s, d], a2r.at[s, d], ident)) for d, ident in over_y]
            run(out_cps)
            return out_cps

        def solve(s, cps):
            arrive(cps)
            hi, lo = tree((ar2[s, 8 + d], jnp.zeros((1, 128), jnp.float32)) for d in range(n_gy))
            hi = jnp.broadcast_to(hi, (8, 128))
            lo = jnp.broadcast_to(lo, (8, 128))
            th = jnp.sum(jnp.where(lane == sub, hi, 0.0), axis=1, keepdims=True)
            tl = jnp.sum(jnp.where(lane == sub, lo, jnp.where(lane == sub + 8, hi, 0.0)), axis=1, keepdims=True)
            th = jnp.broadcast_to(th, (8, 128))
            tl = jnp.broadcast_to(tl, (8, 128))
            mu = [quick(jnp.broadcast_to(th[i:i + 1], (8, 128)), jnp.broadcast_to(tl[i:i + 1], (8, 128))) for i in range(8)]
            return coefficients(mu)

        def source(x, r):
            return kb[1, x, pl.ds(r, 8), :]

        first_x = spread_x(0, powers(source))

        tiles = []
        for c in range(2):
            for t in OWN:
                acc = jnp.zeros((8, 128), jnp.float32)
                for q in range(3):
                    x = 4 + 2 * q + c
                    k = kb[0, x, pl.ds(8 * t, 8), :]
                    for i, get in enumerate((source, r1, r2, r3)):
                        at_lane = i * 8 + q
                        acc = jnp.where(lane == at_lane, pltpu.roll(k * get(x, 8 * t), at_lane + 1, 1), acc)
                tiles.append(acc)
        zt[...] = jnp.concatenate(tiles, axis=0).T[0:32, :]

        first_y = spread_y(0, first_x)

        for k, dy, ok, ident in mates:
            @pl.when(ok)
            def _(k=k, dy=dy, ident=ident):
                remote(spb.at[8], surf.at[1 + dy, k], sus.at[0, 0], sur.at[1 + dy, k], ident).wait_recv()
        rows = []
        for s in range(3):
            a = jnp.zeros((8, 128), jnp.float32)
            for k in range(7):
                a = jnp.where(sub == k, jnp.broadcast_to(surf[s, k], (8, 128)), a)
            rows.append(a)
        rows.append(jnp.zeros((104, 128), jnp.float32))
        mt[...] = jnp.concatenate(rows, axis=0).T
        for k in range(7):
            for c in range(2):
                x = 2 * k + c
                for t in WIDE:
                    if t == 1:
                        r, at_lane = c * 64 + 56, k
                    elif t == 10:
                        r, at_lane = c * 64, 16 + k
                    else:
                        r, at_lane = c * 64 + 8 * (t - 2), 8 + k
                    p = pltpu.roll(mt[r:r + 8, :], 127 - at_lane, 1)
                    k8 = kb[0, x, pl.ds(8 * t, 8), :]
                    b2[x, pl.ds(8 * t, 8), :] = kb[1, x, pl.ds(8 * t, 8), :] + jnp.where(l127, k8 * (0.5 * p), 0.0)

        second_x = spread_x(1, powers(reader(b2)))
        second_y = spread_y(1, second_x)
        c1 = solve(0, first_y)
        flow_in = c1[0] * zt[0:8, :]
        for i in range(1, 4):
            flow_in = flow_in + c1[i] * zt[8 * i:8 * i + 8, :]
        for q in range(3):
            infs[8 + q] = flow_in[q:q + 1, :]
        tells = []
        for k, dy, ok, ident in mates:
            dm = (1, 1, 0, 0, 0, -1, -1)[k]
            tells.append((ok, remote(infs.at[8:11], infl.at[1 - dy, dm + 1], ins.at[k * 3 + dy + 1], inr.at[1 - dy, dm + 1], ident)))
        run(tells)
        c2 = solve(1, second_y)

        for x in range(4, 10):
            for t in OWN:
                rows8 = pl.ds(8 * t, 8)
                total = (c2[0] * b2[x, rows8, :] + c2[1] * v1[x, rows8, :]) + (c2[2] * v2[x, rows8, :] + c2[3] * v3[x, rows8, :])
                out[(x - 4) // 2, x % 2, pl.ds(8 * t - 16, 8), :] = total
        drain(pending + first_x + first_y + second_x + second_y + tells)


def solution(mesh):
    n_grp, n_gx, n_gy = mesh.shape["grp"], mesh.shape["gx"], mesh.shape["gy"]

    def per_device(drive, permeability):
        vmem = lambda *shape: pltpu.VMEM(shape, jnp.float32)
        dma = lambda *shape: pltpu.SemaphoreType.DMA(shape)
        return pl.pallas_call(
            functools.partial(kernel, n_grp, n_gx, n_gy),
            out_shape=jax.ShapeDtypeStruct(drive.shape, jnp.float32),
            in_specs=[pl.BlockSpec(memory_space=pltpu.HBM)] * 2,
            out_specs=pl.BlockSpec(memory_space=pltpu.VMEM),
            scratch_shapes=[
                vmem(3, 6, ROWS, 128), vmem(4, 6, ROWS, 128), vmem(4, 6, ROWS, 128),
                vmem(4, 6, ROWS, 128), vmem(4, 6, ROWS, 128),
                vmem(2, 14, ROWS, 128), vmem(3, 14, ROWS, 128),
                vmem(14, ROWS, 128), vmem(14, ROWS, 128), vmem(14, ROWS, 128), vmem(14, ROWS, 128),
                vmem(128, 128), vmem(32, 128),
                vmem(4, 8, 1, 128), vmem(24, 1, 128), vmem(4, 3, 3, 1, 128), vmem(24, 1, 128),
                vmem(2, 8, 2, 8, 128), vmem(2, 32, 1, 128), vmem(4, 5, 9, 1, 128), vmem(32, 1, 128),
                dma(4), dma(5, 9), dma(5, 9), dma(2, 8), dma(2, 8), dma(2, 16), dma(2, 16),
                dma(3, 7), dma(3, 7), dma(21), dma(3, 3), dma(3, 5), dma(3, 5),
                pltpu.SemaphoreType.REGULAR((3, 2)), pltpu.SemaphoreType.REGULAR((3, 3)),
            ],
            compiler_params=pltpu.CompilerParams(collective_id=0, has_side_effects=True),
            name="coupling",
        )(drive, permeability)

    return jax.shard_map(
        per_device,
        mesh=mesh,
        in_specs=(P(None, ("grp", "gx"), "gy", None), P("gx", "gy", None)),
        out_specs=P(None, ("grp", "gx"), "gy", None),
        check_vma=False,
    )
```

```python
import functools
import jax
import jax.numpy as jnp
from jax import lax
from jax.experimental import pallas as pl
from jax.experimental.pallas import tpu as pltpu
from jax.sharding import PartitionSpec as P

MESH = pl.DeviceIdType.MESH
C = 0.8 / 6.0
CC = (0.8 / 6.0) * (0.8 / 6.0)
SCALE = 1.0 / 16.0
ROWS = 96
OWN = range(2, 10)
WIDE = range(1, 11)


def loop(lo, hi, body, carry):
    for x in range(lo, hi):
        carry = body(x, carry)
    return carry


def two_sum(a, b):
    s = a + b
    bb = s - a
    return s, (a - (s - bb)) + (b - bb)


def quick(a, b):
    s = a + b
    return s, b - (s - a)


def halves(a):
    t = a * 4097.0
    hi = t - (t - a)
    return hi, a - hi


def two_prod(a, b):
    p = a * b
    ah, al = halves(a)
    bh, bl = halves(b)
    return p, ((ah * bh - p) + ah * bl + al * bh) + al * bl


def dadd(a, b):
    s, e = two_sum(a[0], b[0])
    return quick(s, e + (a[1] + b[1]))


def dsub(a, b):
    return dadd(a, (-b[0], -b[1]))


def dmul(a, b):
    p, e = two_prod(a[0], b[0])
    return quick(p, e + (a[0] * b[1] + a[1] * b[0]))


def drecip(a):
    r = 1.0 / a[0]
    p, pe = two_prod(r, a[0])
    e = ((1.0 - p) - pe) - r * a[1]
    return quick(r, r * e)


def tree(pairs):
    pairs = list(pairs)
    while len(pairs) > 1:
        nxt = []
        for i in range(0, len(pairs) - 1, 2):
            (ah, al), (bh, bl) = pairs[i], pairs[i + 1]
            s, e = two_sum(ah, bh)
            nxt.append((s, e + (al + bl)))
        if len(pairs) % 2:
            nxt.append(pairs[-1])
        pairs = nxt
    return pairs[0]


def coefficients(mu):
    n = 4
    m = [[mu[i + j + 1] for j in range(n)] for i in range(n)]
    y = [mu[i] for i in range(n)]
    low = [[None] * n for _ in range(n)]
    inv = [None] * n
    for k in range(n):
        good = m[k][k][0] > 1e-12 * mu[2 * k + 1][0]
        safe = jnp.where(good, m[k][k][0], 1.0)
        rh, rl = drecip((safe, m[k][k][1]))
        inv[k] = (jnp.where(good, rh, 0.0), jnp.where(good, rl, 0.0))
        for i in range(k + 1, n):
            low[i][k] = dmul(m[i][k], inv[k])
        for i in range(k + 1, n):
            for j in range(k + 1, i + 1):
                m[i][j] = dsub(m[i][j], dmul(low[i][k], m[j][k]))
                m[j][i] = m[i][j]
            y[i] = dsub(y[i], dmul(low[i][k], y[k]))
    c = [None] * n
    for k in range(n - 1, -1, -1):
        s = dmul(y[k], inv[k])
        for i in range(k + 1, n):
            s = dsub(s, dmul(low[i][k], c[i]))
        c[k] = s
    return [v[0] * SCALE for v in c]


def kernel(n_grp, n_gx, n_gy, drive, perm, out, fb, e2, e3, e4, tmp, kb, w, v1, v2, v3, b2, mt, zt,
           surf, spb, infl, infs, ar1, ar2, nb, nbs,
           lsem, hs, hr, a1s, a1r, a2s, a2r, sus, sur, ins, inr, ns, nr, fs, fr, tok, ready):
    grp = lax.axis_index("grp")
    gx = lax.axis_index("gx")
    gy = lax.axis_index("gy")
    flows = (n_grp - 1) * n_gx
    is_bed = grp == n_grp - 1
    j = grp * n_gx + gx
    m_of = lax.div(j, 3)
    r_of = j - 3 * m_of
    lane = lax.broadcasted_iota(jnp.int32, (8, 128), 1)
    sub = lax.broadcasted_iota(jnp.int32, (8, 128), 0)
    l0 = lane == 0
    l127 = lane == 127

    def inside(i, n):
        return (i >= 0) & (i < n)

    def held(i, n):
        return jnp.minimum(jnp.maximum(i, 0), n - 1)

    def at(flow):
        flow = held(flow, flows)
        return (lax.div(flow, n_gx), lax.rem(flow, n_gx))

    def below(f):
        return jnp.where(l0, 0.0, pltpu.roll(f, 1, 1))

    def above(f):
        return jnp.where(l127, 0.0, pltpu.roll(f, 127, 1))

    barrier = pltpu.get_barrier_semaphore()
    dirs = [(dx, dy) for dx in (-1, 0, 1) for dy in (-1, 0, 1) if (dx, dy) != (0, 0)]

    def greet(partners):
        total = jnp.int32(0)
        for ok, ident in partners:
            @pl.when(ok)
            def _(ident=ident):
                pl.semaphore_signal(barrier, inc=1, device_id=ident, device_id_type=MESH)
            total = total + ok.astype(jnp.int32)
        return total

    def run(copies):
        for ok, cp in copies:
            @pl.when(ok)
            def _(cp=cp):
                cp.start()

    def arrive(copies):
        for ok, cp in copies:
            @pl.when(ok)
            def _(cp=cp):
                cp.wait_recv()

    def drain(copies):
        for ok, cp in copies:
            @pl.when(ok)
            def _(cp=cp):
                cp.wait_send()

    def remote(src, dst, s, r, ident):
        return pltpu.make_async_remote_copy(src_ref=src, dst_ref=dst, send_sem=s, recv_sem=r,
                                            device_id=ident, device_id_type=MESH)

    def halo(e, view, first, width, wide, neighbour, exists, corners):
        sends, recvs = [], []
        for dx, dy in dirs:
            if not corners and dx != 0 and dy != 0:
                continue
            if dx == 0:
                sc, dc = (first, width), (first, width)
            elif dx == 1:
                sc, dc = (first + width - wide, wide), (first - wide, wide)
            else:
                sc, dc = (first, wide), (first + width, wide)
            if dy == 0:
                sr, dr = (16, 64), (16, 64)
            elif dy == 1:
                sr, dr = (72, 8), (8, 8)
            else:
                sr, dr = (16, 8), (80, 8)
            d = (dx + 1) * 3 + dy + 1
            cp = remote(view(sc, sr), view(dc, dr), hs.at[e, d], hr.at[e, d], neighbour(dx, dy))
            sends.append((exists(dx, dy), cp))
            recvs.append((exists(-dx, -dy), remote(view(sc, sr), view(dc, dr), hs.at[e, d], hr.at[e, d],
                                                   neighbour(-dx, -dy))))
        return sends, recvs

    @pl.when(jnp.logical_not(is_bed))
    def _():
        infl[...] = jnp.zeros_like(infl)
        nb[...] = jnp.zeros_like(nb)
        load = pltpu.make_async_copy(drive, fb.at[:, 4:6, 16:80, :], lsem.at[0])
        load.start()

        def neighbour(dx, dy):
            a, b = at(j + dx)
            return (a, b, held(gy + dy, n_gy))

        def exists(dx, dy):
            return inside(j + dx, flows) & inside(gy + dy, n_gy)

        beds = []
        for dm in (-1, 0, 1):
            for dy in (-1, 0, 1):
                ok = inside(m_of + dm, n_gx) & inside(gy + dy, n_gy)
                if dm == -1:
                    ok = ok & (r_of <= 1)
                if dm == 1:
                    ok = ok & (r_of >= 1)
                beds.append((dm, dy, ok, (n_grp - 1, held(m_of + dm, n_gx), held(gy + dy, n_gy))))

        around = [(o, dy) for o in (-2, 2, -1, 1, 0) for dy in (-1, 1, 0) if (o, dy) != (0, 0)]
        total = greet([(exists(o, dy), neighbour(o, dy)) for o, dy in around])
        greet([(ok, ident) for _, _, ok, ident in beds])

        def clear(bufs, c0, c1, r0, r1):
            for buf in bufs:
                buf[:, c0:c1, r0:r1, :] = jnp.zeros((buf.shape[0], c1 - c0, r1 - r0, 128), jnp.float32)

        @pl.when(j <= 1)
        def _():
            clear((fb,), 1, 2, 8, 88)

        @pl.when(j == 0)
        def _():
            clear((fb,), 2, 4, 8, 88)
            clear((e3, e4), 0, 2, 8, 88)

        @pl.when(j >= flows - 2)
        def _():
            clear((fb,), 8, 9, 8, 88)

        @pl.when(j == flows - 1)
        def _():
            clear((fb,), 6, 8, 8, 88)
            clear((e3, e4), 4, 6, 8, 88)

        @pl.when(gy == 0)
        def _():
            clear((fb,), 1, 9, 8, 16)
            clear((e3, e4), 0, 6, 8, 16)

        @pl.when(gy == n_gy - 1)
        def _():
            clear((fb,), 1, 9, 80, 88)
            clear((e3, e4), 0, 6, 80, 88)

        load.wait()

        tiles = []
        for c in range(2):
            for t in OWN:
                acc = fb[0, 4 + c, 8 * t:8 * t + 8, :]
                for f in (1, 2):
                    acc = jnp.where(lane >= 3 * f, pltpu.roll(fb[f, 4 + c, 8 * t:8 * t + 8, :], 3 * f, 1), acc)
                tiles.append(acc)
        turned = jnp.concatenate(tiles, axis=0).T
        for q in range(9):
            nbs[8 + q] = turned[q:q + 1, :]
        pl.semaphore_wait(barrier, total)
        low_out, low_in = [], []
        for o, dy in around:
            low_out.append((exists(o, dy), remote(nbs.at[8:17], nb.at[1 - dy, 2 - o], ns.at[dy + 1, o + 2],
                                                  nr.at[1 - dy, 2 - o], neighbour(o, dy))))
            low_in.append((exists(o, dy), remote(nbs.at[8:17], nb.at[1 + dy, 2 + o], ns.at[dy + 1, o + 2],
                                                 nr.at[1 + dy, 2 + o], neighbour(o, dy))))
        run(low_out)

        def exchange(e, buf, wide, corners):
            view = lambda c, r: buf.at[:, pl.ds(*c), pl.ds(*r), :]
            sends, recvs = halo(e, view, 2, 2, wide, neighbour, exists, corners)
            run(sends)
            arrive(recvs)
            return sends

        sends0, recvs0 = [], []
        for o, dy in around:
            if abs(o) == 2 and dy != 0:
                continue
            sc, dc = {-2: ((4, 1), (8, 1)), -1: ((4, 2), (6, 2)), 0: ((4, 2), (4, 2)),
                      1: ((4, 2), (2, 2)), 2: ((5, 1), (1, 1))}[o]
            sr, dr = {-1: ((16, 8), (80, 8)), 0: ((16, 64), (16, 64)), 1: ((72, 8), (8, 8))}[dy]
            src = fb.at[:, pl.ds(*sc), pl.ds(*sr), :]
            dst = fb.at[:, pl.ds(*dc), pl.ds(*dr), :]
            pair = fs.at[dy + 1, o + 2], fr.at[dy + 1, o + 2]
            sends0.append((exists(o, dy), remote(src, dst, *pair, neighbour(o, dy))))
            recvs0.append((exists(-o, -dy), remote(src, dst, *pair, neighbour(-o, -dy))))
        run(sends0)
        pending = sends0 + low_out

        even = lax.rem(sub, 2) == 0
        column = j * 2 - 3 + sub
        live = (column >= 0) & (column < 2 * flows)
        live = live & ((lane >= 32) | (gy > 0)) & ((lane < 96) | (gy < n_gy - 1))

        def assemble(row):
            rows = []
            for i in range(3):
                a = row(i, -2)
                for o in range(-1, 3):
                    a = jnp.where(sub >= 2 * o + 3, row(i, o), a)
                rows.append((pltpu.roll(a, 32, 1), pltpu.roll(a, 96, 1)))
            middle = jnp.where(even, rows[1][1], rows[1][0])
            south = jnp.where(even, rows[0][0], rows[0][1])
            north = jnp.where(even, rows[2][0], rows[2][1])
            whole = jnp.where(lane < 32, south, jnp.where(lane < 96, middle, north))
            return jnp.where(live, whole, 0.0)

        def plus(a, b):
            return b if a is None else (a if b is None else a + b)

        def minus(a, b):
            return a if b is None else (-b if a is None else a - b)

        def side(a, k):
            if a is None:
                return None
            return (pltpu.roll(a, 1, 0), pltpu.roll(a, 7, 0), pltpu.roll(a, 1, 1), pltpu.roll(a, 127, 1))[k]

        def evolve(fields, inflow, force, n_velocity, n_pressure):
            new = [[None] * 6 for _ in range(4)]
            for z in range(max(n_velocity, n_pressure)):
                div = None
                for f in range(3):
                    c = fields[f][z]
                    if z > 0:
                        be = fields[f][z - 1]
                    else:
                        be = inflow if f == 2 else None
                    sides = [side(c, k) for k in range(4)]
                    if z < n_velocity:
                        total = plus(plus(be, fields[f][z + 1]), force[f][z])
                        for k in range(4):
                            total = plus(total, sides[k])
                        p = fields[3][z]
                        ahead = (side(p, 1), side(p, 3), fields[3][z + 1])[f]
                        total = plus(minus(total, ahead), p)
                        value = None if total is None else C * total
                        if c is not None:
                            value = plus(value, 0.2 * c)
                        if value is not None:
                            new[f][z] = jnp.where(live, value, 0.0)
                    div = plus(div, minus(c, (sides[0], sides[2], be)[f]))
                if z < n_pressure:
                    value = fields[3][z]
                    if div is not None:
                        value = minus(value, 0.5 * div)
                    if value is not None:
                        new[3][z] = jnp.where(live, value, 0.0)
            return new

        nothing = [[None] * 6 for _ in range(4)]
        arrive(low_in)
        force = [[None] * 6 for _ in range(3)]
        for f in range(3):
            for z in range(3):
                q = 3 * f + z

                def row(i, o, q=q):
                    one = nbs[8 + q] if (i, o) == (1, 0) else nb[i, o + 2, q]
                    return jnp.broadcast_to(one, (8, 128))
                force[f][z] = assemble(row)
        low = evolve(nothing, None, force, 3, 0)
        low = evolve(low, None, force, 2, 2)
        low = evolve(low, None, force, 1, 1)
        low = evolve(low, None, force, 0, 1)[3][0]
        spb[8] = jnp.where(lane[0:1] < 64, pltpu.roll(low, 96, 1)[3:4], pltpu.roll(low, 32, 1)[4:5])
        tells = []
        for dm, dy, ok, ident in beds:
            @pl.when(ok)
            def _(dm=dm, dy=dy):
                pl.semaphore_wait(ready.at[1 + dy, dm + 1], 1)
            for r in range(3):
                slot = r + 2 - 3 * dm
                if 0 <= slot < 7:
                    tells.append((ok & (r_of == r), remote(spb.at[8], surf.at[1 - dy, slot], sus.at[1 - dy, slot],
                                                           sur.at[1 - dy, slot], ident)))
        run(tells)
        pending = pending + tells
        arrive(recvs0)

        def valid(x, t):
            ok = inside(j * 2 + x - 2, 2 * flows)
            if t == 1:
                ok = ok & (gy > 0)
            if t == 10:
                ok = ok & (gy < n_gy - 1)
            return ok

        def near(src, f, x, r):
            return (src[f, x - 1, pl.ds(r, 8), :], src[f, x + 1, pl.ds(r, 8), :],
                    src[f, x, pl.ds(r - 1, 8), :], src[f, x, pl.ds(r + 1, 8), :])

        def first_sweep(dst, cols, tiles):
            def body(x, _):
                for t in tiles:
                    r = 8 * t
                    div = None
                    for f in range(3):
                        c = fb[f, x + 2, pl.ds(r, 8), :]
                        we, ea, so, no = near(fb, f, x + 2, r)
                        be = below(c)
                        total = ((we + ea) + (so + no)) + (be + above(c))
                        dst[f, x, pl.ds(r, 8), :] = jnp.where(valid(x, t), (1.2 * C) * c + CC * total, 0.0)
                        part = c - (we, so, be)[f]
                        div = part if div is None else div + part
                    dst[3, x, pl.ds(r, 8), :] = jnp.where(valid(x, t), (-0.5 * C) * div, 0.0)
                return 0
            loop(cols[0], cols[1], body, 0)

        def sweep(src, put, cols, tiles, masked):
            def body(x, _):
                for t in tiles:
                    r = 8 * t
                    p = src[3, x, pl.ds(r, 8), :]
                    toward = (src[3, x + 1, pl.ds(r, 8), :], src[3, x, pl.ds(r + 1, 8), :], above(p))
                    div = None
                    for f in range(3):
                        c = src[f, x, pl.ds(r, 8), :]
                        we, ea, so, no = near(src, f, x, r)
                        be = below(c)
                        total = ((we + ea) + (so + no)) + (be + above(c))
                        total = total + (fb[f, x + 2, pl.ds(r, 8), :] - (toward[f] - p))
                        new = 0.2 * c + C * total
                        put(f, x, r, jnp.where(valid(x, t), new, 0.0) if masked else new)
                        part = c - (we, so, be)[f]
                        div = part if div is None else div + part
                    new = p - 0.5 * div
                    put(3, x, r, jnp.where(valid(x, t), new, 0.0) if masked else new)
                return 0
            loop(cols[0], cols[1], body, 0)

        def into(buf):
            def put(f, x, r, value):
                buf[f, x, pl.ds(r, 8), :] = value
            return put

        def final(f, x, r, value):
            if f < 3:
                out[f, x - 2, pl.ds(r - 16, 8), :] = value

        first_sweep(tmp, (0, 6), WIDE)
        sweep(tmp, into(e2), (1, 5), WIDE, True)
        sweep(e2, into(e3), (2, 4), OWN, False)

        pending += exchange(2, e3, 2, True)
        sweep(e3, into(tmp), (1, 5), WIDE, True)
        sweep(tmp, into(e4), (2, 4), OWN, False)
        pending += exchange(3, e4, 2, True)
        sweep(e4, into(tmp), (1, 5), WIDE, True)
        sweep(tmp, final, (2, 4), OWN, False)

        for dm, dy, ok, ident in beds:
            @pl.when(ok)
            def _(dm=dm, dy=dy, ident=ident):
                remote(infs.at[8:11], infl.at[1 + dy, dm + 1], ins.at[0], inr.at[1 + dy, dm + 1], ident).wait_recv()

        def row(i, o):
            pick = [jnp.broadcast_to(infl[i, (r + o + 3) // 3, (r + o + 3) % 3], (8, 128)) for r in range(3)]
            return jnp.where(r_of == 0, pick[0], jnp.where(r_of == 1, pick[1], pick[2]))

        inflow = assemble(row)
        fields = nothing
        for step in range(4):
            fields = evolve(fields, inflow, nothing, step + 1, step + 1 if step < 3 else 0)
        stack = []
        for f in range(3):
            for c in range(2):
                acc = jnp.zeros((8, 128), jnp.float32)
                for z in range(4):
                    if fields[f][z] is not None:
                        acc = jnp.where(sub == z, pltpu.roll(fields[f][z], (z - 3 - c) % 8, 0), acc)
                stack.append(acc)
        stack.append(jnp.zeros((80, 128), jnp.float32))
        mt[...] = jnp.concatenate(stack, axis=0).T
        for t in range(8):
            turn = mt[32 + 8 * t:40 + 8 * t, :]
            for f in range(3):
                for c in range(2):
                    add = pltpu.roll(turn, (128 - 8 * (2 * f + c)) % 128, 1)
                    out[f, c, 8 * t:8 * t + 8, :] += jnp.where(lane < 8, add, 0.0)
        drain(pending)

    @pl.when(is_bed)
    def _():
        surf[...] = jnp.zeros_like(surf)
        loads = [pltpu.make_async_copy(perm, kb.at[0, 4:10, 16:80, :], lsem.at[0])]
        for c in range(3):
            loads.append(pltpu.make_async_copy(drive.at[c], kb.at[1, 4 + 2 * c:6 + 2 * c, 16:80, :], lsem.at[1 + c]))
        for cp in loads:
            cp.start()

        def neighbour(dx, dy):
            return (n_grp - 1, held(gx + dx, n_gx), held(gy + dy, n_gy))

        def exists(dx, dy):
            return inside(gx + dx, n_gx) & inside(gy + dy, n_gy)

        always = grp >= 0

        def ring(d):
            return (n_grp - 1, gx, lax.rem(gy + d + n_gy, n_gy))

        over_x = [(d, (n_grp - 1, lax.rem(gx + d, n_gx), gy)) for d in range(1, n_gx)]
        over_y = [(d, (n_grp - 1, gx, lax.rem(gy + d, n_gy))) for d in sorted(range(1, n_gy), key=lambda d: -min(d, n_gy - d))]
        mates = []
        for k in range(7):
            flow = 3 * gx - 2 + k
            for dy in (-1, 0, 1):
                a, b = at(flow)
                mates.append((k, dy, inside(flow, flows) & inside(gy + dy, n_gy), (a, b, held(gy + dy, n_gy))))
        total = greet([(exists(dx, dy), neighbour(dx, dy)) for dx, dy in dirs]
                      + [(always, ident) for _, ident in over_x]
                      + [(always, ring(d)) for d in (-1, 1)])
        for _, _, ok, _ in mates:
            total = total + ok.astype(jnp.int32)

        def clear(c0, c1, r0, r1):
            kb[:, c0:c1, r0:r1, :] = jnp.zeros((2, c1 - c0, r1 - r0, 128), jnp.float32)

        @pl.when(gx == 0)
        def _():
            clear(0, 4, 8, 88)

        @pl.when(gx == n_gx - 1)
        def _():
            clear(10, 14, 8, 88)

        @pl.when(gy == 0)
        def _():
            clear(0, 14, 8, 16)

        @pl.when(gy == n_gy - 1)
        def _():
            clear(0, 14, 80, 88)

        for cp in loads:
            cp.wait()
        pl.semaphore_wait(barrier, total)
        for d in (-1, 1):
            pl.semaphore_signal(tok.at[0, (d + 1) // 2], inc=1, device_id=ring(d), device_id_type=MESH)
        view = lambda c, r: kb.at[:, pl.ds(*c), pl.ds(*r), :]
        pending, recvs = halo(4, view, 4, 6, 4, neighbour, exists, True)
        run(pending)
        for k, dy, ok, ident in mates:
            @pl.when(ok)
            def _(k=k, dy=dy, ident=ident):
                pl.semaphore_signal(ready.at[1 - dy, (1, 1, 0, 0, 0, -1, -1)[k] + 1], inc=1, device_id=ident,
                                    device_id_type=MESH)
        for i, far in enumerate((2, 4)):
            for h in range(2):
                pl.semaphore_wait(tok.at[i, h], 1)
            for h in range(2):
                pl.semaphore_signal(tok.at[i + 1, h], inc=1, device_id=ring((2 * h - 1) * far), device_id_type=MESH)
        arrive(recvs)

        def weight(x, _):
            open_x = gx >= 0
            if x == 3:
                open_x = gx > 0
            if x == 9:
                open_x = gx < n_gx - 1
            for t in WIDE:
                r = 8 * t
                k = kb[0, x, pl.ds(r, 8), :]
                w[0, x, pl.ds(r, 8), :] = jnp.where(open_x, (k + kb[0, x + 1, pl.ds(r, 8), :]) * (0.5 * SCALE), 0.0)
                wy = (k + kb[0, x, pl.ds(r + 1, 8), :]) * (0.5 * SCALE)
                if t == 1:
                    wy = jnp.where((gy == 0) & (sub == 7), 0.0, wy)
                if t == 9:
                    wy = jnp.where((gy == n_gy - 1) & (sub == 7), 0.0, wy)
                w[1, x, pl.ds(r, 8), :] = wy
                up = pltpu.roll(k, 127, 1)
                w[2, x, pl.ds(r, 8), :] = jnp.where(l127, k * SCALE, (k + up) * (0.5 * SCALE))
            return 0

        loop(0, 13, weight, 0)

        def image(src, x, t):
            r = 8 * t
            f = src(x, r)
            ge = w[0, x, pl.ds(r, 8), :] * (f - src(x + 1, r))
            gw = w[0, x - 1, pl.ds(r, 8), :] * (f - src(x - 1, r))
            gn = w[1, x, pl.ds(r, 8), :] * (f - src(x, r + 1))
            gs = w[1, x, pl.ds(r - 1, 8), :] * (f - src(x, r - 1))
            gz = w[2, x, pl.ds(r, 8), :] * (f - above(f))
            return ((ge + gw) + (gn + gs)) + (gz - below(gz))

        def reader(ref):
            return lambda x, r: ref[x, pl.ds(r, 8), :]

        r1, r2, r3 = reader(v1), reader(v2), reader(v3)

        def powers(src):
            for here, there, lo, hi in ((src, v1, 1, 13), (r1, v2, 2, 12), (r2, v3, 3, 11)):
                def body(x, _, here=here, there=there):
                    for t in WIDE:
                        there[x, pl.ds(8 * t, 8), :] = image(here, x, t)
                    return 0
                loop(lo, hi, body, 0)

            def body(x, acc):
                acc = list(acc)
                for t in OWN:
                    v = [get(x, 8 * t) for get in (src, r1, r2, r3)] + [image(r3, x, t)]
                    for i in range(8):
                        s, e = two_sum(acc[2 * i], v[i // 2] * v[(i + 1) // 2])
                        acc[2 * i] = s
                        acc[2 * i + 1] = acc[2 * i + 1] + e
                return tuple(acc)
            acc = loop(4, 10, body, tuple(jnp.zeros((8, 128), jnp.float32) for _ in range(16)))
            level = [(acc[2 * i], acc[2 * i + 1]) for i in range(8)]
            for d in (4, 2, 1):
                keep = (sub & d) == 0
                nxt = []
                for i in range(d):
                    a, b = level[i], level[i + d]
                    x = [jnp.where(keep, a[h], b[h]) for h in range(2)]
                    y = [jnp.where(keep, b[h], a[h]) for h in range(2)]
                    y = [jnp.where(keep, pltpu.roll(q, 8 - d, 0), pltpu.roll(q, d, 0)) for q in y]
                    s, e = two_sum(x[0], y[0])
                    nxt.append((s, e + (x[1] + y[1])))
                level = nxt
            return level[0]

        def spread_x(s, pair):
            ar1[s, 0, 0] = pair[0]
            ar1[s, 0, 1] = pair[1]
            cps = [(always, remote(ar1.at[s, 0], ar1.at[s, d], a1s.at[s, d], a1r.at[s, d], ident)) for d, ident in over_x]
            run(cps)
            return cps

        def spread_y(s, cps):
            arrive(cps)
            hi, lo = tree((ar1[s, d, 0], ar1[s, d, 1]) for d in range(n_gx))
            big = jnp.max(jnp.abs(hi), axis=1, keepdims=True) * 512.0
            top = (hi + big) - big
            th = jnp.sum(top, axis=1, keepdims=True)
            tl = jnp.sum((hi - top) + lo, axis=1, keepdims=True)
            th, tl = two_sum(th, tl)
            spot = jnp.where(lane == sub, th, jnp.where(lane == sub + 8, tl, 0.0))
            ar2[s, 8] = jnp.sum(spot, axis=0, keepdims=True)
            out_cps = [(always, remote(ar2.at[s, 8], ar2.at[s, 8 + d], a2s.at[s, d], a2r.at[s, d], ident)) for d, ident in over_y]
            run(out_cps)
            return out_cps

        def solve(s, cps):
            arrive(cps)
            hi, lo = tree((ar2[s, 8 + d], jnp.zeros((1, 128), jnp.float32)) for d in range(n_gy))
            hi = jnp.broadcast_to(hi, (8, 128))
            lo = jnp.broadcast_to(lo, (8, 128))
            th = jnp.sum(jnp.where(lane == sub, hi, 0.0), axis=1, keepdims=True)
            tl = jnp.sum(jnp.where(lane == sub, lo, jnp.where(lane == sub + 8, hi, 0.0)), axis=1, keepdims=True)
            th = jnp.broadcast_to(th, (8, 128))
            tl = jnp.broadcast_to(tl, (8, 128))
            mu = [quick(jnp.broadcast_to(th[i:i + 1], (8, 128)), jnp.broadcast_to(tl[i:i + 1], (8, 128))) for i in range(8)]
            return coefficients(mu)

        def source(x, r):
            return kb[1, x, pl.ds(r, 8), :]

        first_x = spread_x(0, powers(source))

        tiles = []
        for c in range(2):
            for t in OWN:
                acc = jnp.zeros((8, 128), jnp.float32)
                for q in range(3):
                    x = 4 + 2 * q + c
                    k = kb[0, x, pl.ds(8 * t, 8), :]
                    for i, get in enumerate((source, r1, r2, r3)):
                        at_lane = i * 8 + q
                        acc = jnp.where(lane == at_lane, pltpu.roll(k * get(x, 8 * t), at_lane + 1, 1), acc)
                tiles.append(acc)
        zt[...] = jnp.concatenate(tiles, axis=0).T[0:32, :]

        for h in range(2):
            pl.semaphore_wait(tok.at[2, h], 1)
        first_y = spread_y(0, first_x)

        for k, dy, ok, ident in mates:
            @pl.when(ok)
            def _(k=k, dy=dy, ident=ident):
                remote(spb.at[8], surf.at[1 + dy, k], sus.at[0, 0], sur.at[1 + dy, k], ident).wait_recv()
        rows = []
        for s in range(3):
            a = jnp.zeros((8, 128), jnp.float32)
            for k in range(7):
                a = jnp.where(sub == k, jnp.broadcast_to(surf[s, k], (8, 128)), a)
            rows.append(a)
        rows.append(jnp.zeros((104, 128), jnp.float32))
        mt[...] = jnp.concatenate(rows, axis=0).T
        for k in range(7):
            for c in range(2):
                x = 2 * k + c
                for t in WIDE:
                    if t == 1:
                        r, at_lane = c * 64 + 56, k
                    elif t == 10:
                        r, at_lane = c * 64, 16 + k
                    else:
                        r, at_lane = c * 64 + 8 * (t - 2), 8 + k
                    p = pltpu.roll(mt[r:r + 8, :], 127 - at_lane, 1)
                    k8 = kb[0, x, pl.ds(8 * t, 8), :]
                    b2[x, pl.ds(8 * t, 8), :] = kb[1, x, pl.ds(8 * t, 8), :] + jnp.where(l127, k8 * (0.5 * p), 0.0)

        second_x = spread_x(1, powers(reader(b2)))
        second_y = spread_y(1, second_x)
        c1 = solve(0, first_y)
        flow_in = c1[0] * zt[0:8, :]
        for i in range(1, 4):
            flow_in = flow_in + c1[i] * zt[8 * i:8 * i + 8, :]
        for q in range(3):
            infs[8 + q] = flow_in[q:q + 1, :]
        tells = []
        for k, dy, ok, ident in mates:
            dm = (1, 1, 0, 0, 0, -1, -1)[k]
            tells.append((ok, remote(infs.at[8:11], infl.at[1 - dy, dm + 1], ins.at[k * 3 + dy + 1], inr.at[1 - dy, dm + 1], ident)))
        run(tells)
        c2 = solve(1, second_y)

        for x in range(4, 10):
            for t in OWN:
                rows8 = pl.ds(8 * t, 8)
                total = (c2[0] * b2[x, rows8, :] + c2[1] * v1[x, rows8, :]) + (c2[2] * v2[x, rows8, :] + c2[3] * v3[x, rows8, :])
                out[(x - 4) // 2, x % 2, pl.ds(8 * t - 16, 8), :] = total
        drain(pending + first_x + first_y + second_x + second_y + tells)


def solution(mesh):
    n_grp, n_gx, n_gy = mesh.shape["grp"], mesh.shape["gx"], mesh.shape["gy"]

    def per_device(drive, permeability):
        vmem = lambda *shape: pltpu.VMEM(shape, jnp.float32)
        dma = lambda *shape: pltpu.SemaphoreType.DMA(shape)
        return pl.pallas_call(
            functools.partial(kernel, n_grp, n_gx, n_gy),
            out_shape=jax.ShapeDtypeStruct(drive.shape, jnp.float32),
            in_specs=[pl.BlockSpec(memory_space=pltpu.HBM)] * 2,
            out_specs=pl.BlockSpec(memory_space=pltpu.VMEM),
            scratch_shapes=[
                vmem(3, 10, ROWS, 128), vmem(4, 6, ROWS, 128), vmem(4, 6, ROWS, 128),
                vmem(4, 6, ROWS, 128), vmem(4, 6, ROWS, 128),
                vmem(2, 14, ROWS, 128), vmem(3, 14, ROWS, 128),
                vmem(14, ROWS, 128), vmem(14, ROWS, 128), vmem(14, ROWS, 128), vmem(14, ROWS, 128),
                vmem(128, 128), vmem(32, 128),
                vmem(4, 8, 1, 128), vmem(24, 1, 128), vmem(4, 3, 3, 1, 128), vmem(24, 1, 128),
                vmem(2, 8, 2, 8, 128), vmem(2, 32, 1, 128), vmem(4, 5, 9, 1, 128), vmem(32, 1, 128),
                dma(4), dma(5, 9), dma(5, 9), dma(2, 8), dma(2, 8), dma(2, 16), dma(2, 16),
                dma(3, 7), dma(3, 7), dma(21), dma(3, 3), dma(3, 5), dma(3, 5), dma(3, 5), dma(3, 5),
                pltpu.SemaphoreType.REGULAR((3, 2)), pltpu.SemaphoreType.REGULAR((3, 3)),
            ],
            compiler_params=pltpu.CompilerParams(collective_id=0, has_side_effects=True, vmem_limit_bytes=40 * 1024 * 1024),
            name="coupling",
        )(pltpu.with_memory_space_constraint(drive, pltpu.HBM), pltpu.with_memory_space_constraint(permeability, pltpu.HBM))

    return jax.shard_map(
        per_device,
        mesh=mesh,
        in_specs=(P(None, ("grp", "gx"), "gy", None), P("gx", "gy", None)),
        out_specs=P(None, ("grp", "gx"), "gy", None),
        check_vma=False,
    )
```

```python
import functools
import jax
import jax.numpy as jnp
from jax import lax
from jax.experimental import pallas as pl
from jax.experimental.pallas import tpu as pltpu
from jax.sharding import PartitionSpec as P

MESH = pl.DeviceIdType.MESH
C = 0.8 / 6.0
CC = (0.8 / 6.0) * (0.8 / 6.0)
SCALE = 1.0 / 16.0
ROWS = 96
OWN = range(2, 10)
WIDE = range(1, 11)


def loop(lo, hi, body, carry):
    for x in range(lo, hi):
        carry = body(x, carry)
    return carry


def two_sum(a, b):
    s = a + b
    bb = s - a
    return s, (a - (s - bb)) + (b - bb)


def quick(a, b):
    s = a + b
    return s, b - (s - a)


def halves(a):
    t = a * 4097.0
    hi = t - (t - a)
    return hi, a - hi


def two_prod(a, b):
    p = a * b
    ah, al = halves(a)
    bh, bl = halves(b)
    return p, ((ah * bh - p) + ah * bl + al * bh) + al * bl


def dadd(a, b):
    s, e = two_sum(a[0], b[0])
    return quick(s, e + (a[1] + b[1]))


def dsub(a, b):
    return dadd(a, (-b[0], -b[1]))


def dmul(a, b):
    p, e = two_prod(a[0], b[0])
    return quick(p, e + (a[0] * b[1] + a[1] * b[0]))


def drecip(a):
    r = 1.0 / a[0]
    p, pe = two_prod(r, a[0])
    e = ((1.0 - p) - pe) - r * a[1]
    return quick(r, r * e)


def tree(pairs):
    pairs = list(pairs)
    while len(pairs) > 1:
        nxt = []
        for i in range(0, len(pairs) - 1, 2):
            (ah, al), (bh, bl) = pairs[i], pairs[i + 1]
            s, e = two_sum(ah, bh)
            nxt.append((s, e + (al + bl)))
        if len(pairs) % 2:
            nxt.append(pairs[-1])
        pairs = nxt
    return pairs[0]


def coefficients(mu):
    n = 4
    m = [[mu[i + j + 1] for j in range(n)] for i in range(n)]
    y = [mu[i] for i in range(n)]
    low = [[None] * n for _ in range(n)]
    inv = [None] * n
    for k in range(n):
        good = m[k][k][0] > 1e-12 * mu[2 * k + 1][0]
        safe = jnp.where(good, m[k][k][0], 1.0)
        rh, rl = drecip((safe, m[k][k][1]))
        inv[k] = (jnp.where(good, rh, 0.0), jnp.where(good, rl, 0.0))
        for i in range(k + 1, n):
            low[i][k] = dmul(m[i][k], inv[k])
        for i in range(k + 1, n):
            for j in range(k + 1, i + 1):
                m[i][j] = dsub(m[i][j], dmul(low[i][k], m[j][k]))
                m[j][i] = m[i][j]
            y[i] = dsub(y[i], dmul(low[i][k], y[k]))
    c = [None] * n
    for k in range(n - 1, -1, -1):
        s = dmul(y[k], inv[k])
        for i in range(k + 1, n):
            s = dsub(s, dmul(low[i][k], c[i]))
        c[k] = s
    return [v[0] * SCALE for v in c]


def kernel(n_grp, n_gx, n_gy, drive, perm, out, fb, e2, e3, e4, tmp, kb, w, v1, v2, v3, b2, mt, zt,
           surf, spb, infl, infs, ar1, ar2, nb, nbs,
           lsem, hs, hr, a1s, a1r, a2s, a2r, sus, sur, ins, inr, ns, nr, fs, fr, tok):
    grp = lax.axis_index("grp")
    gx = lax.axis_index("gx")
    gy = lax.axis_index("gy")
    flows = (n_grp - 1) * n_gx
    is_bed = grp == n_grp - 1
    j = grp * n_gx + gx
    m_of = lax.div(j, 3)
    r_of = j - 3 * m_of
    lane = lax.broadcasted_iota(jnp.int32, (8, 128), 1)
    sub = lax.broadcasted_iota(jnp.int32, (8, 128), 0)
    l0 = lane == 0
    l127 = lane == 127

    def inside(i, n):
        return (i >= 0) & (i < n)

    def held(i, n):
        return jnp.minimum(jnp.maximum(i, 0), n - 1)

    def at(flow):
        flow = held(flow, flows)
        return (lax.div(flow, n_gx), lax.rem(flow, n_gx))

    def below(f):
        return jnp.where(l0, 0.0, pltpu.roll(f, 1, 1))

    def above(f):
        return jnp.where(l127, 0.0, pltpu.roll(f, 127, 1))

    barrier = pltpu.get_barrier_semaphore()
    dirs = [(dx, dy) for dx in (-1, 0, 1) for dy in (-1, 0, 1) if (dx, dy) != (0, 0)]

    def greet(partners):
        total = jnp.int32(0)
        for ok, ident in partners:
            @pl.when(ok)
            def _(ident=ident):
                pl.semaphore_signal(barrier, inc=1, device_id=ident, device_id_type=MESH)
            total = total + ok.astype(jnp.int32)
        return total

    def run(copies):
        for ok, cp in copies:
            @pl.when(ok)
            def _(cp=cp):
                cp.start()

    def arrive(copies):
        for ok, cp in copies:
            @pl.when(ok)
            def _(cp=cp):
                cp.wait_recv()

    def drain(copies):
        for ok, cp in copies:
            @pl.when(ok)
            def _(cp=cp):
                cp.wait_send()

    def remote(src, dst, s, r, ident):
        return pltpu.make_async_remote_copy(src_ref=src, dst_ref=dst, send_sem=s, recv_sem=r,
                                            device_id=ident, device_id_type=MESH)

    def halo(e, view, first, width, wide, neighbour, exists, corners):
        sends, recvs = [], []
        for dx, dy in dirs:
            if not corners and dx != 0 and dy != 0:
                continue
            if dx == 0:
                sc, dc = (first, width), (first, width)
            elif dx == 1:
                sc, dc = (first + width - wide, wide), (first - wide, wide)
            else:
                sc, dc = (first, wide), (first + width, wide)
            if dy == 0:
                sr, dr = (16, 64), (16, 64)
            elif dy == 1:
                sr, dr = (72, 8), (8, 8)
            else:
                sr, dr = (16, 8), (80, 8)
            d = (dx + 1) * 3 + dy + 1
            cp = remote(view(sc, sr), view(dc, dr), hs.at[e, d], hr.at[e, d], neighbour(dx, dy))
            sends.append((exists(dx, dy), cp))
            recvs.append((exists(-dx, -dy), remote(view(sc, sr), view(dc, dr), hs.at[e, d], hr.at[e, d],
                                                   neighbour(-dx, -dy))))
        return sends, recvs

    @pl.when(jnp.logical_not(is_bed))
    def _():
        load = pltpu.make_async_copy(drive, fb.at[:, 4:6, 16:80, :], lsem.at[0])
        load.start()

        def neighbour(dx, dy):
            a, b = at(j + dx)
            return (a, b, held(gy + dy, n_gy))

        def exists(dx, dy):
            return inside(j + dx, flows) & inside(gy + dy, n_gy)

        beds = []
        for dm in (-1, 0, 1):
            for dy in (-1, 0, 1):
                ok = inside(m_of + dm, n_gx) & inside(gy + dy, n_gy)
                if dm == -1:
                    ok = ok & (r_of <= 1)
                if dm == 1:
                    ok = ok & (r_of >= 1)
                beds.append((dm, dy, ok, (n_grp - 1, held(m_of + dm, n_gx), held(gy + dy, n_gy))))

        around = [(o, dy) for o in (-2, 2, -1, 1, 0) for dy in (-1, 1, 0) if (o, dy) != (0, 0) and (abs(o) < 2 or dy == 0)]
        total = greet([(exists(o, dy), neighbour(o, dy)) for o, dy in around])
        for _, _, ok, _ in beds:
            total = total + ok.astype(jnp.int32)

        def clear(bufs, c0, c1, r0, r1):
            for buf in bufs:
                buf[:, c0:c1, r0:r1, :] = jnp.zeros((buf.shape[0], c1 - c0, r1 - r0, 128), jnp.float32)

        @pl.when(j <= 1)
        def _():
            clear((fb,), 1, 2, 8, 88)

        @pl.when(j == 0)
        def _():
            clear((fb,), 2, 4, 8, 88)
            clear((e3, e4), 0, 2, 8, 88)

        @pl.when(j >= flows - 2)
        def _():
            clear((fb,), 8, 9, 8, 88)

        @pl.when(j == flows - 1)
        def _():
            clear((fb,), 6, 8, 8, 88)
            clear((e3, e4), 4, 6, 8, 88)

        @pl.when(gy == 0)
        def _():
            clear((fb,), 1, 9, 8, 16)
            clear((e3, e4), 0, 6, 8, 16)

        @pl.when(gy == n_gy - 1)
        def _():
            clear((fb,), 1, 9, 80, 88)
            clear((e3, e4), 0, 6, 80, 88)

        load.wait()

        tiles = []
        for c in range(2):
            for t in OWN:
                acc = fb[0, 4 + c, 8 * t:8 * t + 8, :]
                for f in (1, 2):
                    acc = jnp.where(lane >= 3 * f, pltpu.roll(fb[f, 4 + c, 8 * t:8 * t + 8, :], 3 * f, 1), acc)
                tiles.append(acc)
        turned = jnp.concatenate(tiles, axis=0).T
        for q in range(9):
            nbs[8 + q] = turned[q:q + 1, :]
        pl.semaphore_wait(barrier, total)
        low_out, low_in = [], []
        for o, dy in around:
            low_out.append((exists(o, dy), remote(nbs.at[8:17], nb.at[1 - dy, 2 - o], ns.at[dy + 1, o + 2],
                                                  nr.at[1 - dy, 2 - o], neighbour(o, dy))))
            low_in.append((exists(o, dy), remote(nbs.at[8:17], nb.at[1 + dy, 2 + o], ns.at[dy + 1, o + 2],
                                                 nr.at[1 + dy, 2 + o], neighbour(o, dy))))
        run(low_out)

        def exchange(e, buf, wide, corners):
            view = lambda c, r: buf.at[:, pl.ds(*c), pl.ds(*r), :]
            sends, recvs = halo(e, view, 2, 2, wide, neighbour, exists, corners)
            run(sends)
            arrive(recvs)
            return sends

        sends0, recvs0 = [], []
        for o, dy in around:
            sc, dc = {-2: ((4, 1), (8, 1)), -1: ((4, 2), (6, 2)), 0: ((4, 2), (4, 2)),
                      1: ((4, 2), (2, 2)), 2: ((5, 1), (1, 1))}[o]
            sr, dr = {-1: ((16, 8), (80, 8)), 0: ((16, 64), (16, 64)), 1: ((72, 8), (8, 8))}[dy]
            src = fb.at[:, pl.ds(*sc), pl.ds(*sr), :]
            dst = fb.at[:, pl.ds(*dc), pl.ds(*dr), :]
            pair = fs.at[dy + 1, o + 2], fr.at[dy + 1, o + 2]
            sends0.append((exists(o, dy), remote(src, dst, *pair, neighbour(o, dy))))
            recvs0.append((exists(-o, -dy), remote(src, dst, *pair, neighbour(-o, -dy))))
        run(sends0)
        pending = sends0 + low_out

        even = lax.rem(sub, 2) == 0
        column = j * 2 - 3 + sub
        live = (column >= 0) & (column < 2 * flows)
        live = live & ((lane >= 32) | (gy > 0)) & ((lane < 96) | (gy < n_gy - 1))

        def assemble(row):
            rows = []
            for i in range(3):
                a = row(i, -2)
                for o in range(-1, 3):
                    a = jnp.where(sub >= 2 * o + 3, row(i, o), a)
                rows.append((pltpu.roll(a, 32, 1), pltpu.roll(a, 96, 1)))
            middle = jnp.where(even, rows[1][1], rows[1][0])
            south = jnp.where(even, rows[0][0], rows[0][1])
            north = jnp.where(even, rows[2][0], rows[2][1])
            whole = jnp.where(lane < 32, south, jnp.where(lane < 96, middle, north))
            return jnp.where(live, whole, 0.0)

        def plus(a, b):
            return b if a is None else (a if b is None else a + b)

        def minus(a, b):
            return a if b is None else (-b if a is None else a - b)

        def side(a, k):
            if a is None:
                return None
            return (pltpu.roll(a, 1, 0), pltpu.roll(a, 7, 0), pltpu.roll(a, 1, 1), pltpu.roll(a, 127, 1))[k]

        def evolve(fields, inflow, force, n_velocity, n_pressure):
            new = [[None] * 6 for _ in range(4)]
            for z in range(max(n_velocity, n_pressure)):
                div = None
                for f in range(3):
                    c = fields[f][z]
                    if z > 0:
                        be = fields[f][z - 1]
                    else:
                        be = inflow if f == 2 else None
                    sides = [side(c, k) for k in range(4)]
                    if z < n_velocity:
                        total = plus(plus(be, fields[f][z + 1]), force[f][z])
                        for k in range(4):
                            total = plus(total, sides[k])
                        p = fields[3][z]
                        ahead = (side(p, 1), side(p, 3), fields[3][z + 1])[f]
                        total = plus(minus(total, ahead), p)
                        value = None if total is None else C * total
                        if c is not None:
                            value = plus(value, 0.2 * c)
                        if value is not None:
                            new[f][z] = jnp.where(live, value, 0.0)
                    div = plus(div, minus(c, (sides[0], sides[2], be)[f]))
                if z < n_pressure:
                    value = fields[3][z]
                    if div is not None:
                        value = minus(value, 0.5 * div)
                    if value is not None:
                        new[3][z] = jnp.where(live, value, 0.0)
            return new

        nothing = [[None] * 6 for _ in range(4)]
        arrive(low_in)
        force = [[None] * 6 for _ in range(3)]
        for f in range(3):
            for z in range(3):
                q = 3 * f + z

                def row(i, o, q=q):
                    if abs(o) == 2 and i != 1:
                        return jnp.zeros((8, 128), jnp.float32)
                    one = nbs[8 + q] if (i, o) == (1, 0) else nb[i, o + 2, q]
                    return jnp.broadcast_to(one, (8, 128))
                force[f][z] = assemble(row)
        low = evolve(nothing, None, force, 3, 0)
        low = evolve(low, None, force, 2, 2)
        low = evolve(low, None, force, 1, 1)
        low = evolve(low, None, force, 0, 1)[3][0]
        spb[8] = jnp.where(lane[0:1] < 64, pltpu.roll(low, 96, 1)[3:4], pltpu.roll(low, 32, 1)[4:5])
        tells = []
        for dm, dy, ok, ident in beds:
            for r in range(3):
                slot = r + 2 - 3 * dm
                if 0 <= slot < 7:
                    tells.append((ok & (r_of == r), remote(spb.at[8], surf.at[1 - dy, slot], sus.at[1 - dy, slot],
                                                           sur.at[1 - dy, slot], ident)))
        run(tells)
        pending = pending + tells
        arrive(recvs0)

        def valid(x, t):
            ok = inside(j * 2 + x - 2, 2 * flows)
            if t == 1:
                ok = ok & (gy > 0)
            if t == 10:
                ok = ok & (gy < n_gy - 1)
            return ok

        def near(src, f, x, r):
            return (src[f, x - 1, pl.ds(r, 8), :], src[f, x + 1, pl.ds(r, 8), :],
                    src[f, x, pl.ds(r - 1, 8), :], src[f, x, pl.ds(r + 1, 8), :])

        def first_sweep(dst, cols, tiles):
            def body(x, _):
                for t in tiles:
                    r = 8 * t
                    div = None
                    for f in range(3):
                        c = fb[f, x + 2, pl.ds(r, 8), :]
                        we, ea, so, no = near(fb, f, x + 2, r)
                        be = below(c)
                        total = ((we + ea) + (so + no)) + (be + above(c))
                        dst[f, x, pl.ds(r, 8), :] = jnp.where(valid(x, t), (1.2 * C) * c + CC * total, 0.0)
                        part = c - (we, so, be)[f]
                        div = part if div is None else div + part
                    dst[3, x, pl.ds(r, 8), :] = jnp.where(valid(x, t), (-0.5 * C) * div, 0.0)
                return 0
            loop(cols[0], cols[1], body, 0)

        def sweep(src, put, cols, tiles, masked):
            def body(x, _):
                for t in tiles:
                    r = 8 * t
                    p = src[3, x, pl.ds(r, 8), :]
                    toward = (src[3, x + 1, pl.ds(r, 8), :], src[3, x, pl.ds(r + 1, 8), :], above(p))
                    div = None
                    for f in range(3):
                        c = src[f, x, pl.ds(r, 8), :]
                        we, ea, so, no = near(src, f, x, r)
                        be = below(c)
                        total = ((we + ea) + (so + no)) + (be + above(c))
                        total = total + (fb[f, x + 2, pl.ds(r, 8), :] - (toward[f] - p))
                        new = 0.2 * c + C * total
                        put(f, x, r, jnp.where(valid(x, t), new, 0.0) if masked else new)
                        part = c - (we, so, be)[f]
                        div = part if div is None else div + part
                    new = p - 0.5 * div
                    put(3, x, r, jnp.where(valid(x, t), new, 0.0) if masked else new)
                return 0
            loop(cols[0], cols[1], body, 0)

        def into(buf):
            def put(f, x, r, value):
                buf[f, x, pl.ds(r, 8), :] = value
            return put

        def final(f, x, r, value):
            if f < 3:
                out[f, x - 2, pl.ds(r - 16, 8), :] = value

        first_sweep(tmp, (0, 6), WIDE)
        sweep(tmp, into(e2), (1, 5), WIDE, True)
        sweep(e2, into(e3), (2, 4), OWN, False)

        pending += exchange(2, e3, 2, True)
        sweep(e3, into(tmp), (1, 5), WIDE, True)
        sweep(tmp, into(e4), (2, 4), OWN, False)
        pending += exchange(3, e4, 2, True)
        sweep(e4, into(tmp), (1, 5), WIDE, True)
        sweep(tmp, final, (2, 4), OWN, False)

        for dm, dy, ok, ident in beds:
            @pl.when(ok if dm == 0 or dy == 0 else ok & (r_of != 1))
            def _(dm=dm, dy=dy, ident=ident):
                remote(infs.at[8:11], infl.at[1 + dy, dm + 1], ins.at[0], inr.at[1 + dy, dm + 1], ident).wait_recv()

        def row(i, o):
            if abs(o) == 2 and i != 1:
                return jnp.zeros((8, 128), jnp.float32)
            pick = [jnp.broadcast_to(infl[i, (r + o + 3) // 3, (r + o + 3) % 3], (8, 128)) for r in range(3)]
            return jnp.where(r_of == 0, pick[0], jnp.where(r_of == 1, pick[1], pick[2]))

        inflow = assemble(row)
        fields = nothing
        for step in range(4):
            fields = evolve(fields, inflow, nothing, step + 1, step + 1 if step < 3 else 0)
        stack = []
        for f in range(3):
            for c in range(2):
                acc = jnp.zeros((8, 128), jnp.float32)
                for z in range(4):
                    if fields[f][z] is not None:
                        acc = jnp.where(sub == z, pltpu.roll(fields[f][z], (z - 3 - c) % 8, 0), acc)
                stack.append(acc)
        stack.append(jnp.zeros((80, 128), jnp.float32))
        mt[...] = jnp.concatenate(stack, axis=0).T
        for t in range(8):
            turn = mt[32 + 8 * t:40 + 8 * t, :]
            for f in range(3):
                for c in range(2):
                    add = pltpu.roll(turn, (128 - 8 * (2 * f + c)) % 128, 1)
                    out[f, c, 8 * t:8 * t + 8, :] += jnp.where(lane < 8, add, 0.0)
        drain(pending)

    @pl.when(is_bed)
    def _():
        surf[...] = jnp.zeros_like(surf)
        loads = [pltpu.make_async_copy(perm, kb.at[0, 4:10, 16:80, :], lsem.at[0])]
        for c in range(3):
            loads.append(pltpu.make_async_copy(drive.at[c], kb.at[1, 4 + 2 * c:6 + 2 * c, 16:80, :], lsem.at[1 + c]))
        for cp in loads:
            cp.start()

        def neighbour(dx, dy):
            return (n_grp - 1, held(gx + dx, n_gx), held(gy + dy, n_gy))

        def exists(dx, dy):
            return inside(gx + dx, n_gx) & inside(gy + dy, n_gy)

        always = grp >= 0

        def ring(d):
            return (n_grp - 1, gx, lax.rem(gy + d + n_gy, n_gy))

        over_x = [(d, (n_grp - 1, lax.rem(gx + d, n_gx), gy)) for d in range(1, n_gx)]
        over_y = [(d, (n_grp - 1, gx, lax.rem(gy + d, n_gy))) for d in sorted(range(1, n_gy), key=lambda d: -min(d, n_gy - d))]
        mates = []
        for k in range(7):
            flow = 3 * gx - 2 + k
            for dy in (-1, 0, 1):
                a, b = at(flow)
                mates.append((k, dy, inside(flow, flows) & inside(gy + dy, n_gy), (a, b, held(gy + dy, n_gy))))
        total = greet([(exists(dx, dy), neighbour(dx, dy)) for dx, dy in dirs]
                      + [(always, ident) for _, ident in over_x]
                      + [(always, ring(d)) for d in (-1, 1)])
        greet([(ok, ident) for _, _, ok, ident in mates])

        def clear(c0, c1, r0, r1):
            kb[:, c0:c1, r0:r1, :] = jnp.zeros((2, c1 - c0, r1 - r0, 128), jnp.float32)

        @pl.when(gx == 0)
        def _():
            clear(0, 4, 8, 88)

        @pl.when(gx == n_gx - 1)
        def _():
            clear(10, 14, 8, 88)

        @pl.when(gy == 0)
        def _():
            clear(0, 14, 8, 16)

        @pl.when(gy == n_gy - 1)
        def _():
            clear(0, 14, 80, 88)

        for cp in loads:
            cp.wait()
        pl.semaphore_wait(barrier, total)
        for d in (-1, 1):
            pl.semaphore_signal(tok.at[0, (d + 1) // 2], inc=1, device_id=ring(d), device_id_type=MESH)
        view = lambda c, r: kb.at[:, pl.ds(*c), pl.ds(*r), :]
        pending, recvs = halo(4, view, 4, 6, 4, neighbour, exists, True)
        run(pending)
        for i, far in enumerate((2, 4)):
            for h in range(2):
                pl.semaphore_wait(tok.at[i, h], 1)
            for h in range(2):
                pl.semaphore_signal(tok.at[i + 1, h], inc=1, device_id=ring((2 * h - 1) * far), device_id_type=MESH)
        arrive(recvs)

        def weight(x, _):
            open_x = gx >= 0
            if x == 3:
                open_x = gx > 0
            if x == 9:
                open_x = gx < n_gx - 1
            for t in WIDE:
                r = 8 * t
                k = kb[0, x, pl.ds(r, 8), :]
                w[0, x, pl.ds(r, 8), :] = jnp.where(open_x, (k + kb[0, x + 1, pl.ds(r, 8), :]) * (0.5 * SCALE), 0.0)
                wy = (k + kb[0, x, pl.ds(r + 1, 8), :]) * (0.5 * SCALE)
                if t == 1:
                    wy = jnp.where((gy == 0) & (sub == 7), 0.0, wy)
                if t == 9:
                    wy = jnp.where((gy == n_gy - 1) & (sub == 7), 0.0, wy)
                w[1, x, pl.ds(r, 8), :] = wy
                up = pltpu.roll(k, 127, 1)
                w[2, x, pl.ds(r, 8), :] = jnp.where(l127, k * SCALE, (k + up) * (0.5 * SCALE))
            return 0

        loop(0, 13, weight, 0)

        def image(src, x, t):
            r = 8 * t
            f = src(x, r)
            ge = w[0, x, pl.ds(r, 8), :] * (f - src(x + 1, r))
            gw = w[0, x - 1, pl.ds(r, 8), :] * (f - src(x - 1, r))
            gn = w[1, x, pl.ds(r, 8), :] * (f - src(x, r + 1))
            gs = w[1, x, pl.ds(r - 1, 8), :] * (f - src(x, r - 1))
            gz = w[2, x, pl.ds(r, 8), :] * (f - above(f))
            return ((ge + gw) + (gn + gs)) + (gz - below(gz))

        def reader(ref):
            return lambda x, r: ref[x, pl.ds(r, 8), :]

        r1, r2, r3 = reader(v1), reader(v2), reader(v3)

        def powers(src):
            for here, there, lo, hi in ((src, v1, 1, 13), (r1, v2, 2, 12), (r2, v3, 3, 11)):
                def body(x, _, here=here, there=there):
                    for t in WIDE:
                        there[x, pl.ds(8 * t, 8), :] = image(here, x, t)
                    return 0
                loop(lo, hi, body, 0)

            def body(x, acc):
                acc = list(acc)
                for t in OWN:
                    v = [get(x, 8 * t) for get in (src, r1, r2, r3)] + [image(r3, x, t)]
                    for i in range(8):
                        s, e = two_sum(acc[2 * i], v[i // 2] * v[(i + 1) // 2])
                        acc[2 * i] = s
                        acc[2 * i + 1] = acc[2 * i + 1] + e
                return tuple(acc)
            acc = loop(4, 10, body, tuple(jnp.zeros((8, 128), jnp.float32) for _ in range(16)))
            level = [(acc[2 * i], acc[2 * i + 1]) for i in range(8)]
            for d in (4, 2, 1):
                keep = (sub & d) == 0
                nxt = []
                for i in range(d):
                    a, b = level[i], level[i + d]
                    x = [jnp.where(keep, a[h], b[h]) for h in range(2)]
                    y = [jnp.where(keep, b[h], a[h]) for h in range(2)]
                    y = [jnp.where(keep, pltpu.roll(q, 8 - d, 0), pltpu.roll(q, d, 0)) for q in y]
                    s, e = two_sum(x[0], y[0])
                    nxt.append((s, e + (x[1] + y[1])))
                level = nxt
            return level[0]

        def spread_x(s, pair):
            ar1[s, 0, 0] = pair[0]
            ar1[s, 0, 1] = pair[1]
            cps = [(always, remote(ar1.at[s, 0], ar1.at[s, d], a1s.at[s, d], a1r.at[s, d], ident)) for d, ident in over_x]
            run(cps)
            return cps

        def spread_y(s, cps):
            arrive(cps)
            hi, lo = tree((ar1[s, d, 0], ar1[s, d, 1]) for d in range(n_gx))
            big = jnp.max(jnp.abs(hi), axis=1, keepdims=True) * 512.0
            top = (hi + big) - big
            th = jnp.sum(top, axis=1, keepdims=True)
            tl = jnp.sum((hi - top) + lo, axis=1, keepdims=True)
            th, tl = two_sum(th, tl)
            spot = jnp.where(lane == sub, th, jnp.where(lane == sub + 8, tl, 0.0))
            ar2[s, 8] = jnp.sum(spot, axis=0, keepdims=True)
            out_cps = [(always, remote(ar2.at[s, 8], ar2.at[s, 8 + d], a2s.at[s, d], a2r.at[s, d], ident)) for d, ident in over_y]
            run(out_cps)
            return out_cps

        def solve(s, cps):
            arrive(cps)
            hi, lo = tree((ar2[s, 8 + d], jnp.zeros((1, 128), jnp.float32)) for d in range(n_gy))
            hi = jnp.broadcast_to(hi, (8, 128))
            lo = jnp.broadcast_to(lo, (8, 128))
            th = jnp.sum(jnp.where(lane == sub, hi, 0.0), axis=1, keepdims=True)
            tl = jnp.sum(jnp.where(lane == sub, lo, jnp.where(lane == sub + 8, hi, 0.0)), axis=1, keepdims=True)
            th = jnp.broadcast_to(th, (8, 128))
            tl = jnp.broadcast_to(tl, (8, 128))
            mu = [quick(jnp.broadcast_to(th[i:i + 1], (8, 128)), jnp.broadcast_to(tl[i:i + 1], (8, 128))) for i in range(8)]
            return coefficients(mu)

        def source(x, r):
            return kb[1, x, pl.ds(r, 8), :]

        first_x = spread_x(0, powers(source))

        tiles = []
        for c in range(2):
            for t in OWN:
                acc = jnp.zeros((8, 128), jnp.float32)
                for q in range(3):
                    x = 4 + 2 * q + c
                    k = kb[0, x, pl.ds(8 * t, 8), :]
                    for i, get in enumerate((source, r1, r2, r3)):
                        at_lane = i * 8 + q
                        acc = jnp.where(lane == at_lane, pltpu.roll(k * get(x, 8 * t), at_lane + 1, 1), acc)
                tiles.append(acc)
        zt[...] = jnp.concatenate(tiles, axis=0).T[0:32, :]

        for h in range(2):
            pl.semaphore_wait(tok.at[2, h], 1)
        first_y = spread_y(0, first_x)

        for k, dy, ok, ident in mates:
            @pl.when(ok)
            def _(k=k, dy=dy, ident=ident):
                remote(spb.at[8], surf.at[1 + dy, k], sus.at[0, 0], sur.at[1 + dy, k], ident).wait_recv()
        rows = []
        for s in range(3):
            a = jnp.zeros((8, 128), jnp.float32)
            for k in range(7):
                a = jnp.where(sub == k, jnp.broadcast_to(surf[s, k], (8, 128)), a)
            rows.append(a)
        rows.append(jnp.zeros((104, 128), jnp.float32))
        mt[...] = jnp.concatenate(rows, axis=0).T
        for k in range(7):
            for c in range(2):
                x = 2 * k + c
                for t in WIDE:
                    if t == 1:
                        r, at_lane = c * 64 + 56, k
                    elif t == 10:
                        r, at_lane = c * 64, 16 + k
                    else:
                        r, at_lane = c * 64 + 8 * (t - 2), 8 + k
                    p = pltpu.roll(mt[r:r + 8, :], 127 - at_lane, 1)
                    k8 = kb[0, x, pl.ds(8 * t, 8), :]
                    b2[x, pl.ds(8 * t, 8), :] = kb[1, x, pl.ds(8 * t, 8), :] + jnp.where(l127, k8 * (0.5 * p), 0.0)

        second_x = spread_x(1, powers(reader(b2)))
        second_y = spread_y(1, second_x)
        c1 = solve(0, first_y)
        flow_in = c1[0] * zt[0:8, :]
        for i in range(1, 4):
            flow_in = flow_in + c1[i] * zt[8 * i:8 * i + 8, :]
        for q in range(3):
            infs[8 + q] = flow_in[q:q + 1, :]
        tells = []
        for k, dy, ok, ident in mates:
            dm = (1, 1, 0, 0, 0, -1, -1)[k]
            if k in (0, 6) and dy != 0:
                continue
            tells.append((ok, remote(infs.at[8:11], infl.at[1 - dy, dm + 1], ins.at[k * 3 + dy + 1], inr.at[1 - dy, dm + 1], ident)))
        run(tells)
        c2 = solve(1, second_y)

        for x in range(4, 10):
            for t in OWN:
                rows8 = pl.ds(8 * t, 8)
                total = (c2[0] * b2[x, rows8, :] + c2[1] * v1[x, rows8, :]) + (c2[2] * v2[x, rows8, :] + c2[3] * v3[x, rows8, :])
                out[(x - 4) // 2, x % 2, pl.ds(8 * t - 16, 8), :] = total
        drain(pending + first_x + first_y + second_x + second_y + tells)


def solution(mesh):
    n_grp, n_gx, n_gy = mesh.shape["grp"], mesh.shape["gx"], mesh.shape["gy"]

    def per_device(drive, permeability):
        vmem = lambda *shape: pltpu.VMEM(shape, jnp.float32)
        dma = lambda *shape: pltpu.SemaphoreType.DMA(shape)
        return pl.pallas_call(
            functools.partial(kernel, n_grp, n_gx, n_gy),
            out_shape=jax.ShapeDtypeStruct(drive.shape, jnp.float32),
            in_specs=[pl.BlockSpec(memory_space=pltpu.HBM)] * 2,
            out_specs=pl.BlockSpec(memory_space=pltpu.VMEM),
            scratch_shapes=[
                vmem(3, 10, ROWS, 128), vmem(4, 6, ROWS, 128), vmem(4, 6, ROWS, 128),
                vmem(4, 6, ROWS, 128), vmem(4, 6, ROWS, 128),
                vmem(2, 14, ROWS, 128), vmem(3, 14, ROWS, 128),
                vmem(14, ROWS, 128), vmem(14, ROWS, 128), vmem(14, ROWS, 128), vmem(14, ROWS, 128),
                vmem(128, 128), vmem(32, 128),
                vmem(4, 8, 1, 128), vmem(24, 1, 128), vmem(4, 3, 3, 1, 128), vmem(24, 1, 128),
                vmem(2, 8, 2, 8, 128), vmem(2, 32, 1, 128), vmem(4, 5, 9, 1, 128), vmem(32, 1, 128),
                dma(4), dma(5, 9), dma(5, 9), dma(2, 8), dma(2, 8), dma(2, 16), dma(2, 16),
                dma(3, 7), dma(3, 7), dma(21), dma(3, 3), dma(3, 5), dma(3, 5), dma(3, 5), dma(3, 5),
                pltpu.SemaphoreType.REGULAR((3, 2)),
            ],
            compiler_params=pltpu.CompilerParams(collective_id=0, has_side_effects=True, vmem_limit_bytes=40 * 1024 * 1024),
            name="coupling",
        )(pltpu.with_memory_space_constraint(drive, pltpu.HBM), pltpu.with_memory_space_constraint(permeability, pltpu.HBM))

    return jax.shard_map(
        per_device,
        mesh=mesh,
        in_specs=(P(None, ("grp", "gx"), "gy", None), P("gx", "gy", None)),
        out_specs=P(None, ("grp", "gx"), "gy", None),
        check_vma=False,
    )
```

```python
import functools
import jax
import jax.numpy as jnp
from jax import lax
from jax.experimental import pallas as pl
from jax.experimental.pallas import tpu as pltpu
from jax.sharding import PartitionSpec as P

MESH = pl.DeviceIdType.MESH
C = 0.8 / 6.0
CC = (0.8 / 6.0) * (0.8 / 6.0)
SCALE = 1.0 / 16.0
ROWS = 96
OWN = range(2, 10)
WIDE = range(1, 11)


def loop(lo, hi, body, carry):
    for x in range(lo, hi):
        carry = body(x, carry)
    return carry


def two_sum(a, b):
    s = a + b
    bb = s - a
    return s, (a - (s - bb)) + (b - bb)


def quick(a, b):
    s = a + b
    return s, b - (s - a)


def halves(a):
    t = a * 4097.0
    hi = t - (t - a)
    return hi, a - hi


def two_prod(a, b):
    p = a * b
    ah, al = halves(a)
    bh, bl = halves(b)
    return p, ((ah * bh - p) + ah * bl + al * bh) + al * bl


def dadd(a, b):
    s, e = two_sum(a[0], b[0])
    return quick(s, e + (a[1] + b[1]))


def dsub(a, b):
    return dadd(a, (-b[0], -b[1]))


def dmul(a, b):
    p, e = two_prod(a[0], b[0])
    return quick(p, e + (a[0] * b[1] + a[1] * b[0]))


def drecip(a):
    r = 1.0 / a[0]
    p, pe = two_prod(r, a[0])
    e = ((1.0 - p) - pe) - r * a[1]
    return quick(r, r * e)


def tree(pairs):
    pairs = list(pairs)
    while len(pairs) > 1:
        nxt = []
        for i in range(0, len(pairs) - 1, 2):
            (ah, al), (bh, bl) = pairs[i], pairs[i + 1]
            s, e = two_sum(ah, bh)
            nxt.append((s, e + (al + bl)))
        if len(pairs) % 2:
            nxt.append(pairs[-1])
        pairs = nxt
    return pairs[0]


def coefficients(mu):
    n = 4
    m = [[mu[i + j + 1] for j in range(n)] for i in range(n)]
    y = [mu[i] for i in range(n)]
    low = [[None] * n for _ in range(n)]
    inv = [None] * n
    for k in range(n):
        good = m[k][k][0] > 1e-12 * mu[2 * k + 1][0]
        safe = jnp.where(good, m[k][k][0], 1.0)
        rh, rl = drecip((safe, m[k][k][1]))
        inv[k] = (jnp.where(good, rh, 0.0), jnp.where(good, rl, 0.0))
        for i in range(k + 1, n):
            low[i][k] = dmul(m[i][k], inv[k])
        for i in range(k + 1, n):
            for j in range(k + 1, i + 1):
                m[i][j] = dsub(m[i][j], dmul(low[i][k], m[j][k]))
                m[j][i] = m[i][j]
            y[i] = dsub(y[i], dmul(low[i][k], y[k]))
    c = [None] * n
    for k in range(n - 1, -1, -1):
        s = dmul(y[k], inv[k])
        for i in range(k + 1, n):
            s = dsub(s, dmul(low[i][k], c[i]))
        c[k] = s
    return [v[0] * SCALE for v in c]


def kernel(n_grp, n_gx, n_gy, drive, perm, out, fb, e2, e3, e4, tmp, kb, w, v1, v2, v3, b2, mt, zt,
           surf, spb, infl, infs, ar1, ar2, nb, nbs,
           lsem, hs, hr, a1s, a1r, a2s, a2r, sus, sur, ins, inr, ns, nr, fs, fr, tok):
    grp = lax.axis_index("grp")
    gx = lax.axis_index("gx")
    gy = lax.axis_index("gy")
    flows = (n_grp - 1) * n_gx
    is_bed = grp == n_grp - 1
    j = grp * n_gx + gx
    m_of = lax.div(j, 3)
    r_of = j - 3 * m_of
    lane = lax.broadcasted_iota(jnp.int32, (8, 128), 1)
    sub = lax.broadcasted_iota(jnp.int32, (8, 128), 0)
    l0 = lane == 0
    l127 = lane == 127

    def inside(i, n):
        return (i >= 0) & (i < n)

    def held(i, n):
        return jnp.minimum(jnp.maximum(i, 0), n - 1)

    def at(flow):
        flow = held(flow, flows)
        return (lax.div(flow, n_gx), lax.rem(flow, n_gx))

    def below(f):
        return jnp.where(l0, 0.0, pltpu.roll(f, 1, 1))

    def above(f):
        return jnp.where(l127, 0.0, pltpu.roll(f, 127, 1))

    barrier = pltpu.get_barrier_semaphore()
    dirs = [(dx, dy) for dx in (-1, 0, 1) for dy in (-1, 0, 1) if (dx, dy) != (0, 0)]

    def greet(partners):
        total = jnp.int32(0)
        for ok, ident in partners:
            @pl.when(ok)
            def _(ident=ident):
                pl.semaphore_signal(barrier, inc=1, device_id=ident, device_id_type=MESH)
            total = total + ok.astype(jnp.int32)
        return total

    def run(copies):
        for ok, cp in copies:
            @pl.when(ok)
            def _(cp=cp):
                cp.start()

    def arrive(copies):
        for ok, cp in copies:
            @pl.when(ok)
            def _(cp=cp):
                cp.wait_recv()

    def drain(copies):
        for ok, cp in copies:
            @pl.when(ok)
            def _(cp=cp):
                cp.wait_send()

    def remote(src, dst, s, r, ident):
        return pltpu.make_async_remote_copy(src_ref=src, dst_ref=dst, send_sem=s, recv_sem=r,
                                            device_id=ident, device_id_type=MESH)

    def halo(e, view, first, width, wide, neighbour, exists, corners):
        sends, recvs = [], []
        for dx, dy in dirs:
            if not corners and dx != 0 and dy != 0:
                continue
            if dx == 0:
                sc, dc = (first, width), (first, width)
            elif dx == 1:
                sc, dc = (first + width - wide, wide), (first - wide, wide)
            else:
                sc, dc = (first, wide), (first + width, wide)
            if dy == 0:
                sr, dr = (16, 64), (16, 64)
            elif dy == 1:
                sr, dr = (72, 8), (8, 8)
            else:
                sr, dr = (16, 8), (80, 8)
            d = (dx + 1) * 3 + dy + 1
            cp = remote(view(sc, sr), view(dc, dr), hs.at[e, d], hr.at[e, d], neighbour(dx, dy))
            sends.append((exists(dx, dy), cp))
            recvs.append((exists(-dx, -dy), remote(view(sc, sr), view(dc, dr), hs.at[e, d], hr.at[e, d],
                                                   neighbour(-dx, -dy))))
        return sends, recvs

    @pl.when(jnp.logical_not(is_bed))
    def _():
        load = pltpu.make_async_copy(drive, fb.at[:, 4:6, 16:80, :], lsem.at[0])
        load.start()

        def neighbour(dx, dy):
            a, b = at(j + dx)
            return (a, b, held(gy + dy, n_gy))

        def exists(dx, dy):
            return inside(j + dx, flows) & inside(gy + dy, n_gy)

        beds = []
        for dm in (-1, 0, 1):
            for dy in (-1, 0, 1):
                ok = inside(m_of + dm, n_gx) & inside(gy + dy, n_gy)
                if dm == -1:
                    ok = ok & (r_of <= 1)
                if dm == 1:
                    ok = ok & (r_of >= 1)
                beds.append((dm, dy, ok, (n_grp - 1, held(m_of + dm, n_gx), held(gy + dy, n_gy))))

        around = [(o, dy) for o in (-2, 2, -1, 1, 0) for dy in (-1, 1, 0) if (o, dy) != (0, 0) and (abs(o) < 2 or dy == 0)]
        total = greet([(exists(o, dy), neighbour(o, dy)) for o, dy in around])
        for _, _, ok, _ in beds:
            total = total + ok.astype(jnp.int32)

        def clear(bufs, c0, c1, r0, r1):
            for buf in bufs:
                buf[:, c0:c1, r0:r1, :] = jnp.zeros((buf.shape[0], c1 - c0, r1 - r0, 128), jnp.float32)

        @pl.when(j <= 1)
        def _():
            clear((fb,), 1, 2, 8, 88)

        @pl.when(j == 0)
        def _():
            clear((fb,), 2, 4, 8, 88)
            clear((e3, e4), 0, 2, 8, 88)

        @pl.when(j >= flows - 2)
        def _():
            clear((fb,), 8, 9, 8, 88)

        @pl.when(j == flows - 1)
        def _():
            clear((fb,), 6, 8, 8, 88)
            clear((e3, e4), 4, 6, 8, 88)

        @pl.when(gy == 0)
        def _():
            clear((fb,), 1, 9, 8, 16)
            clear((e3, e4), 0, 6, 8, 16)

        @pl.when(gy == n_gy - 1)
        def _():
            clear((fb,), 1, 9, 80, 88)
            clear((e3, e4), 0, 6, 80, 88)

        load.wait()

        tiles = []
        for c in range(2):
            for t in OWN:
                acc = fb[0, 4 + c, 8 * t:8 * t + 8, :]
                for f in (1, 2):
                    acc = jnp.where(lane >= 3 * f, pltpu.roll(fb[f, 4 + c, 8 * t:8 * t + 8, :], 3 * f, 1), acc)
                tiles.append(acc)
        turned = jnp.concatenate(tiles, axis=0).T
        for q in range(9):
            nbs[8 + q] = turned[q:q + 1, :]
        pl.semaphore_wait(barrier, total)
        low_out, low_in = [], []
        for o, dy in around:
            low_out.append((exists(o, dy), remote(nbs.at[8:17], nb.at[1 - dy, 2 - o], ns.at[dy + 1, o + 2],
                                                  nr.at[1 - dy, 2 - o], neighbour(o, dy))))
            low_in.append((exists(o, dy), remote(nbs.at[8:17], nb.at[1 + dy, 2 + o], ns.at[dy + 1, o + 2],
                                                 nr.at[1 + dy, 2 + o], neighbour(o, dy))))
        run(low_out)

        def exchange(e, buf, wide, corners):
            view = lambda c, r: buf.at[:, pl.ds(*c), pl.ds(*r), :]
            sends, recvs = halo(e, view, 2, 2, wide, neighbour, exists, corners)
            run(sends)
            arrive(recvs)
            return sends

        sends0, recvs0 = [], []
        for o, dy in around:
            sc, dc = {-2: ((4, 1), (8, 1)), -1: ((4, 2), (6, 2)), 0: ((4, 2), (4, 2)),
                      1: ((4, 2), (2, 2)), 2: ((5, 1), (1, 1))}[o]
            sr, dr = {-1: ((16, 8), (80, 8)), 0: ((16, 64), (16, 64)), 1: ((72, 8), (8, 8))}[dy]
            src = fb.at[:, pl.ds(*sc), pl.ds(*sr), :]
            dst = fb.at[:, pl.ds(*dc), pl.ds(*dr), :]
            pair = fs.at[dy + 1, o + 2], fr.at[dy + 1, o + 2]
            sends0.append((exists(o, dy), remote(src, dst, *pair, neighbour(o, dy))))
            recvs0.append((exists(-o, -dy), remote(src, dst, *pair, neighbour(-o, -dy))))
        run(sends0)
        pending = sends0 + low_out

        even = lax.rem(sub, 2) == 0
        column = j * 2 - 3 + sub
        live = (column >= 0) & (column < 2 * flows)
        live = live & ((lane >= 32) | (gy > 0)) & ((lane < 96) | (gy < n_gy - 1))

        def assemble(row):
            rows = []
            for i in range(3):
                a = row(i, -2)
                for o in range(-1, 3):
                    a = jnp.where(sub >= 2 * o + 3, row(i, o), a)
                rows.append((pltpu.roll(a, 32, 1), pltpu.roll(a, 96, 1)))
            middle = jnp.where(even, rows[1][1], rows[1][0])
            south = jnp.where(even, rows[0][0], rows[0][1])
            north = jnp.where(even, rows[2][0], rows[2][1])
            whole = jnp.where(lane < 32, south, jnp.where(lane < 96, middle, north))
            return jnp.where(live, whole, 0.0)

        def plus(a, b):
            return b if a is None else (a if b is None else a + b)

        def minus(a, b):
            return a if b is None else (-b if a is None else a - b)

        def side(a, k):
            if a is None:
                return None
            return (pltpu.roll(a, 1, 0), pltpu.roll(a, 7, 0), pltpu.roll(a, 1, 1), pltpu.roll(a, 127, 1))[k]

        def evolve(fields, inflow, force, n_velocity, n_pressure):
            new = [[None] * 6 for _ in range(4)]
            for z in range(max(n_velocity, n_pressure)):
                div = None
                for f in range(3):
                    c = fields[f][z]
                    if z > 0:
                        be = fields[f][z - 1]
                    else:
                        be = inflow if f == 2 else None
                    sides = [side(c, k) for k in range(4)]
                    if z < n_velocity:
                        total = plus(plus(be, fields[f][z + 1]), force[f][z])
                        for k in range(4):
                            total = plus(total, sides[k])
                        p = fields[3][z]
                        ahead = (side(p, 1), side(p, 3), fields[3][z + 1])[f]
                        total = plus(minus(total, ahead), p)
                        value = None if total is None else C * total
                        if c is not None:
                            value = plus(value, 0.2 * c)
                        if value is not None:
                            new[f][z] = jnp.where(live, value, 0.0)
                    div = plus(div, minus(c, (sides[0], sides[2], be)[f]))
                if z < n_pressure:
                    value = fields[3][z]
                    if div is not None:
                        value = minus(value, 0.5 * div)
                    if value is not None:
                        new[3][z] = jnp.where(live, value, 0.0)
            return new

        nothing = [[None] * 6 for _ in range(4)]
        arrive(low_in)
        force = [[None] * 6 for _ in range(3)]
        for f in range(3):
            for z in range(3):
                q = 3 * f + z

                def row(i, o, q=q):
                    if abs(o) == 2 and i != 1:
                        return jnp.zeros((8, 128), jnp.float32)
                    one = nbs[8 + q] if (i, o) == (1, 0) else nb[i, o + 2, q]
                    return jnp.broadcast_to(one, (8, 128))
                force[f][z] = assemble(row)
        low = evolve(nothing, None, force, 3, 0)
        low = evolve(low, None, force, 2, 2)
        low = evolve(low, None, force, 1, 1)
        low = evolve(low, None, force, 0, 1)[3][0]
        spb[8] = jnp.where(lane[0:1] < 64, pltpu.roll(low, 96, 1)[3:4], pltpu.roll(low, 32, 1)[4:5])
        tells = []
        for dm, dy, ok, ident in beds:
            for r in range(3):
                slot = r + 2 - 3 * dm
                if 0 <= slot < 7:
                    tells.append((ok & (r_of == r), remote(spb.at[8], surf.at[1 - dy, slot], sus.at[1 - dy, slot],
                                                           sur.at[1 - dy, slot], ident)))
        run(tells)
        pending = pending + tells
        arrive(recvs0)

        def valid(x, t):
            ok = inside(j * 2 + x - 2, 2 * flows)
            if t == 1:
                ok = ok & (gy > 0)
            if t == 10:
                ok = ok & (gy < n_gy - 1)
            return ok

        def near(src, f, x, r):
            return (src[f, x - 1, pl.ds(r, 8), :], src[f, x + 1, pl.ds(r, 8), :],
                    src[f, x, pl.ds(r - 1, 8), :], src[f, x, pl.ds(r + 1, 8), :])

        def first_sweep(dst, cols, tiles):
            def body(x, _):
                for t in tiles:
                    r = 8 * t
                    div = None
                    for f in range(3):
                        c = fb[f, x + 2, pl.ds(r, 8), :]
                        we, ea, so, no = near(fb, f, x + 2, r)
                        be = below(c)
                        total = ((we + ea) + (so + no)) + (be + above(c))
                        dst[f, x, pl.ds(r, 8), :] = jnp.where(valid(x, t), (1.2 * C) * c + CC * total, 0.0)
                        part = c - (we, so, be)[f]
                        div = part if div is None else div + part
                    dst[3, x, pl.ds(r, 8), :] = jnp.where(valid(x, t), (-0.5 * C) * div, 0.0)
                return 0
            loop(cols[0], cols[1], body, 0)

        def sweep(src, put, cols, tiles, masked):
            def body(x, _):
                for t in tiles:
                    r = 8 * t
                    p = src[3, x, pl.ds(r, 8), :]
                    toward = (src[3, x + 1, pl.ds(r, 8), :], src[3, x, pl.ds(r + 1, 8), :], above(p))
                    div = None
                    for f in range(3):
                        c = src[f, x, pl.ds(r, 8), :]
                        we, ea, so, no = near(src, f, x, r)
                        be = below(c)
                        total = ((we + ea) + (so + no)) + (be + above(c))
                        total = total + (fb[f, x + 2, pl.ds(r, 8), :] - (toward[f] - p))
                        new = 0.2 * c + C * total
                        put(f, x, r, jnp.where(valid(x, t), new, 0.0) if masked else new)
                        part = c - (we, so, be)[f]
                        div = part if div is None else div + part
                    new = p - 0.5 * div
                    put(3, x, r, jnp.where(valid(x, t), new, 0.0) if masked else new)
                return 0
            loop(cols[0], cols[1], body, 0)

        def into(buf):
            def put(f, x, r, value):
                buf[f, x, pl.ds(r, 8), :] = value
            return put

        def final(f, x, r, value):
            if f < 3:
                out[f, x - 2, pl.ds(r - 16, 8), :] = value

        first_sweep(tmp, (0, 6), WIDE)
        sweep(tmp, into(e2), (1, 5), WIDE, True)
        sweep(e2, into(e3), (2, 4), OWN, False)

        pending += exchange(2, e3, 2, True)
        sweep(e3, into(tmp), (1, 5), WIDE, True)
        sweep(tmp, into(e4), (2, 4), OWN, False)
        pending += exchange(3, e4, 2, True)
        sweep(e4, into(tmp), (1, 5), WIDE, True)
        sweep(tmp, final, (2, 4), OWN, False)

        drain(pending)
        for dm, dy, ok, ident in beds:
            @pl.when(ok if dm == 0 or dy == 0 else ok & (r_of != 1))
            def _(dm=dm, dy=dy, ident=ident):
                remote(infs.at[8:11], infl.at[1 + dy, dm + 1], ins.at[0], inr.at[1 + dy, dm + 1], ident).wait_recv()

        def row(i, o):
            if abs(o) == 2 and i != 1:
                return jnp.zeros((8, 128), jnp.float32)
            pick = [jnp.broadcast_to(infl[i, (r + o + 3) // 3, (r + o + 3) % 3], (8, 128)) for r in range(3)]
            return jnp.where(r_of == 0, pick[0], jnp.where(r_of == 1, pick[1], pick[2]))

        inflow = assemble(row)
        fields = nothing
        for step in range(4):
            fields = evolve(fields, inflow, nothing, step + 1, step + 1 if step < 3 else 0)
        stack = []
        for f in range(3):
            for c in range(2):
                acc = jnp.zeros((8, 128), jnp.float32)
                for z in range(4):
                    if fields[f][z] is not None:
                        acc = jnp.where(sub == z, pltpu.roll(fields[f][z], (z - 3 - c) % 8, 0), acc)
                stack.append(acc)
        stack.append(jnp.zeros((80, 128), jnp.float32))
        mt[...] = jnp.concatenate(stack, axis=0).T
        for t in range(8):
            turn = mt[32 + 8 * t:40 + 8 * t, :]
            for f in range(3):
                for c in range(2):
                    add = pltpu.roll(turn, (128 - 8 * (2 * f + c)) % 128, 1)
                    out[f, c, 8 * t:8 * t + 8, :] += jnp.where(lane < 8, add, 0.0)

    @pl.when(is_bed)
    def _():
        surf[...] = jnp.zeros_like(surf)
        loads = [pltpu.make_async_copy(perm, kb.at[0, 4:10, 16:80, :], lsem.at[0])]
        for c in range(3):
            loads.append(pltpu.make_async_copy(drive.at[c], kb.at[1, 4 + 2 * c:6 + 2 * c, 16:80, :], lsem.at[1 + c]))
        for cp in loads:
            cp.start()

        def neighbour(dx, dy):
            return (n_grp - 1, held(gx + dx, n_gx), held(gy + dy, n_gy))

        def exists(dx, dy):
            return inside(gx + dx, n_gx) & inside(gy + dy, n_gy)

        always = grp >= 0

        def ring(d):
            return (n_grp - 1, gx, lax.rem(gy + d + n_gy, n_gy))

        over_x = [(d, (n_grp - 1, lax.rem(gx + d, n_gx), gy)) for d in range(1, n_gx)]
        over_y = [(d, (n_grp - 1, gx, lax.rem(gy + d, n_gy))) for d in sorted(range(1, n_gy), key=lambda d: -min(d, n_gy - d))]
        mates = []
        for k in range(7):
            flow = 3 * gx - 2 + k
            for dy in (-1, 0, 1):
                a, b = at(flow)
                mates.append((k, dy, inside(flow, flows) & inside(gy + dy, n_gy), (a, b, held(gy + dy, n_gy))))
        total = greet([(exists(dx, dy), neighbour(dx, dy)) for dx, dy in dirs]
                      + [(always, ident) for _, ident in over_x]
                      + [(always, ring(d)) for d in (-1, 1)])
        greet([(ok, ident) for _, _, ok, ident in mates])

        def clear(c0, c1, r0, r1):
            kb[:, c0:c1, r0:r1, :] = jnp.zeros((2, c1 - c0, r1 - r0, 128), jnp.float32)

        @pl.when(gx == 0)
        def _():
            clear(0, 4, 8, 88)

        @pl.when(gx == n_gx - 1)
        def _():
            clear(10, 14, 8, 88)

        @pl.when(gy == 0)
        def _():
            clear(0, 14, 8, 16)

        @pl.when(gy == n_gy - 1)
        def _():
            clear(0, 14, 80, 88)

        for cp in loads:
            cp.wait()
        pl.semaphore_wait(barrier, total)
        for d in (-1, 1):
            pl.semaphore_signal(tok.at[0, (d + 1) // 2], inc=1, device_id=ring(d), device_id_type=MESH)
        view = lambda c, r: kb.at[:, pl.ds(*c), pl.ds(*r), :]
        pending, recvs = halo(4, view, 4, 6, 4, neighbour, exists, True)
        run(pending)
        def weight(x, tiles):
            open_x = gx >= 0
            if x == 3:
                open_x = gx > 0
            if x == 9:
                open_x = gx < n_gx - 1
            for t in tiles:
                r = 8 * t
                k = kb[0, x, pl.ds(r, 8), :]
                w[0, x, pl.ds(r, 8), :] = jnp.where(open_x, (k + kb[0, x + 1, pl.ds(r, 8), :]) * (0.5 * SCALE), 0.0)
                wy = (k + kb[0, x, pl.ds(r + 1, 8), :]) * (0.5 * SCALE)
                if t == 1:
                    wy = jnp.where((gy == 0) & (sub == 7), 0.0, wy)
                if t == 9:
                    wy = jnp.where((gy == n_gy - 1) & (sub == 7), 0.0, wy)
                w[1, x, pl.ds(r, 8), :] = wy
                up = pltpu.roll(k, 127, 1)
                w[2, x, pl.ds(r, 8), :] = jnp.where(l127, k * SCALE, (k + up) * (0.5 * SCALE))

        def image(src, x, t):
            r = 8 * t
            f = src(x, r)
            ge = w[0, x, pl.ds(r, 8), :] * (f - src(x + 1, r))
            gw = w[0, x - 1, pl.ds(r, 8), :] * (f - src(x - 1, r))
            gn = w[1, x, pl.ds(r, 8), :] * (f - src(x, r + 1))
            gs = w[1, x, pl.ds(r - 1, 8), :] * (f - src(x, r - 1))
            gz = w[2, x, pl.ds(r, 8), :] * (f - above(f))
            return ((ge + gw) + (gn + gs)) + (gz - below(gz))

        def source(x, r):
            return kb[1, x, pl.ds(r, 8), :]

        early = [(x, t) for x in range(5, 9) for t in range(3, 9)]
        for x in range(4, 9):
            weight(x, range(2, 9))
        for x, t in early:
            v1[x, pl.ds(8 * t, 8), :] = image(source, x, t)

        for i, far in enumerate((2, 4)):
            for h in range(2):
                pl.semaphore_wait(tok.at[i, h], 1)
            for h in range(2):
                pl.semaphore_signal(tok.at[i + 1, h], inc=1, device_id=ring((2 * h - 1) * far), device_id_type=MESH)
        arrive(recvs)

        for x in range(13):
            weight(x, [t for t in WIDE if not (4 <= x < 9 and 2 <= t < 9)])

        def reader(ref):
            return lambda x, r: ref[x, pl.ds(r, 8), :]

        r1, r2, r3 = reader(v1), reader(v2), reader(v3)

        def powers(src, done=()):
            for here, there, lo, hi in ((src, v1, 1, 13), (r1, v2, 2, 12), (r2, v3, 3, 11)):
                def body(x, _, here=here, there=there):
                    for t in WIDE:
                        if there is v1 and (x, t) in done:
                            continue
                        there[x, pl.ds(8 * t, 8), :] = image(here, x, t)
                    return 0
                loop(lo, hi, body, 0)

            def body(x, acc):
                acc = list(acc)
                for t in OWN:
                    v = [get(x, 8 * t) for get in (src, r1, r2, r3)] + [image(r3, x, t)]
                    for i in range(8):
                        s, e = two_sum(acc[2 * i], v[i // 2] * v[(i + 1) // 2])
                        acc[2 * i] = s
                        acc[2 * i + 1] = acc[2 * i + 1] + e
                return tuple(acc)
            acc = loop(4, 10, body, tuple(jnp.zeros((8, 128), jnp.float32) for _ in range(16)))
            level = [(acc[2 * i], acc[2 * i + 1]) for i in range(8)]
            for d in (4, 2, 1):
                keep = (sub & d) == 0
                nxt = []
                for i in range(d):
                    a, b = level[i], level[i + d]
                    x = [jnp.where(keep, a[h], b[h]) for h in range(2)]
                    y = [jnp.where(keep, b[h], a[h]) for h in range(2)]
                    y = [jnp.where(keep, pltpu.roll(q, 8 - d, 0), pltpu.roll(q, d, 0)) for q in y]
                    s, e = two_sum(x[0], y[0])
                    nxt.append((s, e + (x[1] + y[1])))
                level = nxt
            return level[0]

        def spread_x(s, pair):
            ar1[s, 0, 0] = pair[0]
            ar1[s, 0, 1] = pair[1]
            cps = [(always, remote(ar1.at[s, 0], ar1.at[s, d], a1s.at[s, d], a1r.at[s, d], ident)) for d, ident in over_x]
            run(cps)
            return cps

        def spread_y(s, cps):
            arrive(cps)
            hi, lo = tree((ar1[s, d, 0], ar1[s, d, 1]) for d in range(n_gx))
            big = jnp.max(jnp.abs(hi), axis=1, keepdims=True) * 512.0
            top = (hi + big) - big
            th = jnp.sum(top, axis=1, keepdims=True)
            tl = jnp.sum((hi - top) + lo, axis=1, keepdims=True)
            th, tl = two_sum(th, tl)
            spot = jnp.where(lane == sub, th, jnp.where(lane == sub + 8, tl, 0.0))
            ar2[s, 8] = jnp.sum(spot, axis=0, keepdims=True)
            out_cps = [(always, remote(ar2.at[s, 8], ar2.at[s, 8 + d], a2s.at[s, d], a2r.at[s, d], ident)) for d, ident in over_y]
            run(out_cps)
            return out_cps

        def solve(s, cps):
            arrive(cps)
            hi, lo = tree((ar2[s, 8 + d], jnp.zeros((1, 128), jnp.float32)) for d in range(n_gy))
            hi = jnp.broadcast_to(hi, (8, 128))
            lo = jnp.broadcast_to(lo, (8, 128))
            th = jnp.sum(jnp.where(lane == sub, hi, 0.0), axis=1, keepdims=True)
            tl = jnp.sum(jnp.where(lane == sub, lo, jnp.where(lane == sub + 8, hi, 0.0)), axis=1, keepdims=True)
            th = jnp.broadcast_to(th, (8, 128))
            tl = jnp.broadcast_to(tl, (8, 128))
            mu = [quick(jnp.broadcast_to(th[i:i + 1], (8, 128)), jnp.broadcast_to(tl[i:i + 1], (8, 128))) for i in range(8)]
            return coefficients(mu)

        first_x = spread_x(0, powers(source, early))

        tiles = []
        for c in range(2):
            for t in OWN:
                acc = jnp.zeros((8, 128), jnp.float32)
                for q in range(3):
                    x = 4 + 2 * q + c
                    k = kb[0, x, pl.ds(8 * t, 8), :]
                    for i, get in enumerate((source, r1, r2, r3)):
                        at_lane = i * 8 + q
                        acc = jnp.where(lane == at_lane, pltpu.roll(k * get(x, 8 * t), at_lane + 1, 1), acc)
                tiles.append(acc)
        zt[...] = jnp.concatenate(tiles, axis=0).T[0:32, :]

        for h in range(2):
            pl.semaphore_wait(tok.at[2, h], 1)
        first_y = spread_y(0, first_x)

        for k, dy, ok, ident in mates:
            @pl.when(ok)
            def _(k=k, dy=dy, ident=ident):
                remote(spb.at[8], surf.at[1 + dy, k], sus.at[0, 0], sur.at[1 + dy, k], ident).wait_recv()
        rows = []
        for s in range(3):
            a = jnp.zeros((8, 128), jnp.float32)
            for k in range(7):
                a = jnp.where(sub == k, jnp.broadcast_to(surf[s, k], (8, 128)), a)
            rows.append(a)
        rows.append(jnp.zeros((104, 128), jnp.float32))
        mt[...] = jnp.concatenate(rows, axis=0).T
        for k in range(7):
            for c in range(2):
                x = 2 * k + c
                for t in WIDE:
                    if t == 1:
                        r, at_lane = c * 64 + 56, k
                    elif t == 10:
                        r, at_lane = c * 64, 16 + k
                    else:
                        r, at_lane = c * 64 + 8 * (t - 2), 8 + k
                    p = pltpu.roll(mt[r:r + 8, :], 127 - at_lane, 1)
                    k8 = kb[0, x, pl.ds(8 * t, 8), :]
                    b2[x, pl.ds(8 * t, 8), :] = kb[1, x, pl.ds(8 * t, 8), :] + jnp.where(l127, k8 * (0.5 * p), 0.0)

        second_x = spread_x(1, powers(reader(b2)))
        second_y = spread_y(1, second_x)
        c1 = solve(0, first_y)
        flow_in = c1[0] * zt[0:8, :]
        for i in range(1, 4):
            flow_in = flow_in + c1[i] * zt[8 * i:8 * i + 8, :]
        for q in range(3):
            infs[8 + q] = flow_in[q:q + 1, :]
        tells = []
        for k, dy, ok, ident in mates:
            dm = (1, 1, 0, 0, 0, -1, -1)[k]
            if k in (0, 6) and dy != 0:
                continue
            tells.append((ok, remote(infs.at[8:11], infl.at[1 - dy, dm + 1], ins.at[k * 3 + dy + 1], inr.at[1 - dy, dm + 1], ident)))
        run(tells)
        drain(pending + first_x + first_y + second_x + second_y + tells)
        c2 = solve(1, second_y)

        for x in range(4, 10):
            for t in OWN:
                rows8 = pl.ds(8 * t, 8)
                total = (c2[0] * b2[x, rows8, :] + c2[1] * v1[x, rows8, :]) + (c2[2] * v2[x, rows8, :] + c2[3] * v3[x, rows8, :])
                out[(x - 4) // 2, x % 2, pl.ds(8 * t - 16, 8), :] = total


def solution(mesh):
    n_grp, n_gx, n_gy = mesh.shape["grp"], mesh.shape["gx"], mesh.shape["gy"]

    def per_device(drive, permeability):
        vmem = lambda *shape: pltpu.VMEM(shape, jnp.float32)
        dma = lambda *shape: pltpu.SemaphoreType.DMA(shape)
        return pl.pallas_call(
            functools.partial(kernel, n_grp, n_gx, n_gy),
            out_shape=jax.ShapeDtypeStruct(drive.shape, jnp.float32),
            in_specs=[pl.BlockSpec(memory_space=pltpu.HBM)] * 2,
            out_specs=pl.BlockSpec(memory_space=pltpu.VMEM),
            scratch_shapes=[
                vmem(3, 10, ROWS, 128), vmem(4, 6, ROWS, 128), vmem(4, 6, ROWS, 128),
                vmem(4, 6, ROWS, 128), vmem(4, 6, ROWS, 128),
                vmem(2, 14, ROWS, 128), vmem(3, 14, ROWS, 128),
                vmem(14, ROWS, 128), vmem(14, ROWS, 128), vmem(14, ROWS, 128), vmem(14, ROWS, 128),
                vmem(128, 128), vmem(32, 128),
                vmem(4, 8, 1, 128), vmem(24, 1, 128), vmem(4, 3, 3, 1, 128), vmem(24, 1, 128),
                vmem(2, 8, 2, 8, 128), vmem(2, 32, 1, 128), vmem(4, 5, 9, 1, 128), vmem(32, 1, 128),
                dma(4), dma(5, 9), dma(5, 9), dma(2, 8), dma(2, 8), dma(2, 16), dma(2, 16),
                dma(3, 7), dma(3, 7), dma(21), dma(3, 3), dma(3, 5), dma(3, 5), dma(3, 5), dma(3, 5),
                pltpu.SemaphoreType.REGULAR((3, 2)),
            ],
            compiler_params=pltpu.CompilerParams(collective_id=0, has_side_effects=True, vmem_limit_bytes=40 * 1024 * 1024),
            name="coupling",
        )(pltpu.with_memory_space_constraint(drive, pltpu.HBM), pltpu.with_memory_space_constraint(permeability, pltpu.HBM))

    return jax.shard_map(
        per_device,
        mesh=mesh,
        in_specs=(P(None, ("grp", "gx"), "gy", None), P("gx", "gy", None)),
        out_specs=P(None, ("grp", "gx"), "gy", None),
        check_vma=False,
    )
```
